256 devices in a mesh: fy: 8 (over x, core), fx: 16 (over y, z_lo), ch: 2 (over z_hi).
Axes of the slice: x: 4, y: 4, z: 8 (z_hi: 2, z_lo: 4; z = z_hi * 4 + z_lo), core: 2. Of those that a mesh axis runs over, the one named last changes fastest.
Arguments:
- image_cube: float32 [64, 1024, 1664], P('ch', 'fx', 'fy'), may hold values from 0 to 2
- data_grad: bfloat16 [64, 1024, 1664], P('ch', 'fx', 'fy'), may hold values from -6 to 6
- dual_coeffs: float32 [64, 1792, 2048], P('ch', 'fx', 'fy'), may hold values from -6 to 6
- reweights: float32 [1792, 2048], P('fx', 'fy'), may hold values from 1 to 40
Outputs:
- image_next: float32 [64, 1024, 1664], P('ch', 'fx', 'fy')
- dual_next: float32 [64, 1792, 2048], P('ch', 'fx', 'fy')
The draws below stay inside these ranges and needn't reach their ends.
All inputs are finite; a program needn't handle non-finite values.
Results may differ from the reference program's by a relative error of at most 0.0003.
Values sent between devices are 32-bit elements; how exact they have to be, the bound alone decides.
A program may use at most 64 MiB of HBM per device.

```python
import math
import jax
import jax.numpy as jnp
import numpy as np
from jax import lax

CH = 64
LEVELS = 2
TX = 64
TY = 208
INTERSECTION = 48
EX = 112
EY = 256
NX = 1024
NY = 1664
N_FY = 8
N_FX = 16


def steps_of(own_key, dims, shards, low, top_value):
    def one(position, blocks):
        steps = jax.random.uniform(jax.random.fold_in(jax.random.fold_in(own_key, 6), position), (blocks,), jnp.float32, low / len(shards), top_value / len(shards))
        return jnp.repeat(jnp.exp(steps), dims[position] // blocks).reshape((-1,) + (1,) * (len(dims) - position - 1))

    factor_of = one(*shards[0])
    for cut in shards[1:]:
        factor_of = factor_of * one(*cut)
    return factor_of


def noise(stream_key, dims, width, limit, pieces=(), kind=jnp.bfloat16):
    loudness = steps_of(stream_key, dims, pieces, -0.22, 0.18) if pieces else 1.0
    array = jax.random.normal(stream_key, dims, jnp.float32) * width * loudness
    return jnp.minimum(jnp.maximum(array, -limit), limit).astype(kind)


def setup_inputs(seed: int = 0) -> dict:
    keys = jax.random.split(jax.random.key(seed), 5)
    return {
        "image_cube": jnp.clip(2.0 * jax.random.uniform(keys[0], (CH, NX, NY), jnp.float32) ** steps_of(keys[0], (CH, NX, NY), ((0, 2), (1, 16), (2, 8)), -0.2, 0.2), 0.0, 2.0),
        "data_grad": noise(keys[1], (CH, NX, NY), 1.0, 6.0, ((0, 2), (1, 16), (2, 8))),
        "dual_coeffs": noise(keys[2], (CH, N_FX * EX, N_FY * EY), 1.0, 6.0, ((0, 2), (1, 16), (2, 8)), jnp.float32),
        "reweights": jnp.clip(jnp.exp(math.log(40.0) - 3.6888795 * jax.random.uniform(keys[3], (N_FX * EX, N_FY * EY), jnp.float32) ** steps_of(keys[3], (N_FX * EX, N_FY * EY), ((0, 16), (1, 8)), -0.2, 0.2)), 1.0, 40.0),
    }


LOW_PASS = [-0.00011747678400228192, 0.0006754494059985568, -0.0003917403729959771, -0.00487035299301066, 0.008746094047015655, 0.013981027917015516, -0.04408825393106472, -0.01736930100202211, 0.128747426620186, 0.00047248457399797254, -0.2840155429624281, -0.015829105256023893, 0.5853546836548691, 0.6756307362980128, 0.3128715909144659, 0.05441584224308161]
TAU_STEP = 0.5
LAMBDA_REG = 1.0
EPSILON = 1e-06

def level_matrix(length):
    halved = length // 2
    taps_count = len(LOW_PASS)
    matrix = np.zeros((length, length))
    for out_row in range(halved):
        for tap_index in range(taps_count):
            column = (2 * out_row + tap_index) % length
            matrix[out_row, column] += LOW_PASS[tap_index]
            matrix[halved + out_row, column] += (-1) ** tap_index * LOW_PASS[taps_count - 1 - tap_index]
    return matrix

def analysis(facet_block, levels):
    result = facet_block
    width_x = facet_block.shape[1]
    width_y = facet_block.shape[2]
    for level_step in range(levels):
        matrix_x = jnp.asarray(level_matrix(width_x), dtype=facet_block.dtype)
        matrix_y = jnp.asarray(level_matrix(width_y), dtype=facet_block.dtype)
        corner_part = result[:, :width_x, :width_y]
        corner_part = jnp.einsum('cxy,vy->cxv', corner_part, matrix_y, precision=lax.Precision.HIGHEST)
        corner_part = jnp.einsum('ux,cxv->cuv', matrix_x, corner_part, precision=lax.Precision.HIGHEST)
        result = result.at[:, :width_x, :width_y].set(corner_part)
        width_x = width_x // 2
        width_y = width_y // 2
    return result

def synthesis(coeff_block, levels):
    result = coeff_block
    for level_step in range(levels - 1, -1, -1):
        width_x = coeff_block.shape[1] // 2 ** level_step
        width_y = coeff_block.shape[2] // 2 ** level_step
        matrix_x = jnp.asarray(level_matrix(width_x), dtype=coeff_block.dtype)
        matrix_y = jnp.asarray(level_matrix(width_y), dtype=coeff_block.dtype)
        corner_part = result[:, :width_x, :width_y]
        corner_part = jnp.einsum('ux,cuv->cxv', matrix_x, corner_part, precision=lax.Precision.HIGHEST)
        corner_part = jnp.einsum('cxv,vy->cxy', corner_part, matrix_y, precision=lax.Precision.HIGHEST)
        result = result.at[:, :width_x, :width_y].set(corner_part)
    return result

def cover_weights(total, tile, intersection, count, float_kind):
    positions = jnp.arange(total, dtype=jnp.int32)
    offsets = positions % tile
    owners = positions // tile
    edge = (offsets >= tile - intersection) & (owners < count - 1)
    return jnp.where(edge, 0.5 ** 0.5, 1.0).astype(float_kind)

def reference(image_cube, data_grad, dual_coeffs, reweights):
    float_kind = image_cube.dtype
    weight_map = cover_weights(NX, TX, INTERSECTION, N_FX, float_kind)[:, None] * cover_weights(NY, TY, INTERSECTION, N_FY, float_kind)[None, :]
    facets = N_FX * N_FY
    anchor = jnp.int32(0)

    def add_facet(facet_number, accumulated):
        col_index = (facet_number // N_FY).astype(jnp.int32)
        row_index = (facet_number % N_FY).astype(jnp.int32)
        coeff_block = lax.dynamic_slice(dual_coeffs, (anchor, col_index * EX, row_index * EY), (CH, EX, EY))
        piece = synthesis(coeff_block, LEVELS)
        start = (anchor, col_index * TX, row_index * TY)
        current = lax.dynamic_slice(accumulated, start, (CH, EX, EY))
        return lax.dynamic_update_slice(accumulated, current + piece, start)
    accumulated = jnp.zeros((CH, NX + INTERSECTION, NY + INTERSECTION), float_kind)
    accumulated = lax.fori_loop(0, facets, add_facet, accumulated)
    adjoint = accumulated[:, INTERSECTION:, INTERSECTION:] * weight_map
    image_next = jnp.maximum(image_cube - TAU_STEP * (data_grad.astype(float_kind) + adjoint), 0.0)
    extrap = (2.0 * image_next - image_cube) * weight_map
    padded = jnp.pad(extrap, ((0, 0), (INTERSECTION, 0), (INTERSECTION, 0)))

    def new_facet(facet_number, result):
        col_index = (facet_number // N_FY).astype(jnp.int32)
        row_index = (facet_number % N_FY).astype(jnp.int32)
        window = lax.dynamic_slice(padded, (anchor, col_index * TX, row_index * TY), (CH, EX, EY))
        place = (anchor, col_index * EX, row_index * EY)
        updated = lax.dynamic_slice(dual_coeffs, place, (CH, EX, EY)) + analysis(window, LEVELS)
        squared_sum = lax.optimization_barrier(jnp.sum(updated * updated, axis=0))
        local_weights = lax.dynamic_slice(reweights, (col_index * EX, row_index * EY), (EX, EY))
        factor = jnp.minimum(1.0, LAMBDA_REG * local_weights / jnp.sqrt(squared_sum + EPSILON))
        return lax.dynamic_update_slice(result, updated * factor[None], place)
    dual_next = lax.fori_loop(0, facets, new_facet, jnp.zeros_like(dual_coeffs))
    return (image_next, dual_next)
```

```python
import functools

import jax
import jax.numpy as jnp
import numpy as np
from jax import lax
from jax.experimental import pallas as pl
from jax.experimental.pallas import tpu as pltpu
from jax.sharding import PartitionSpec as P

LOW_PASS = [
    -0.00011747678400228192,
    0.0006754494059985568,
    -0.0003917403729959771,
    -0.00487035299301066,
    0.008746094047015655,
    0.013981027917015516,
    -0.04408825393106472,
    -0.01736930100202211,
    0.128747426620186,
    0.00047248457399797254,
    -0.2840155429624281,
    -0.015829105256023893,
    0.5853546836548691,
    0.6756307362980128,
    0.3128715909144659,
    0.05441584224308161,
]
TAU_STEP = 0.5
LAMBDA_REG = 1.0
EPSILON = 1e-06
LANES = 128
GROUP = 4
MESH = pl.DeviceIdType.MESH


def level_matrix(length):
    halved = length // 2
    taps_count = len(LOW_PASS)
    matrix = np.zeros((length, length))
    for out_row in range(halved):
        for tap_index in range(taps_count):
            column = (2 * out_row + tap_index) % length
            matrix[out_row, column] += LOW_PASS[tap_index]
            matrix[halved + out_row, column] += (-1) ** tap_index * LOW_PASS[
                taps_count - 1 - tap_index
            ]
    return matrix


def split_np(matrix):
    single = matrix.astype(np.float32)
    high = single.astype(jnp.bfloat16)
    low = (single - high.astype(np.float32)).astype(jnp.bfloat16)
    return np.stack([high, low])


def matrices(ex, ey, border):
    wx, wy = level_matrix(ex), level_matrix(ey)
    hx, hy = ex // 2, ey // 2
    along_y = np.concatenate([level_matrix(hy) @ wy[:hy], wy], axis=0)
    order = np.concatenate([np.arange(border, ey), np.arange(border)])
    along_y = along_y[:, order]
    low_x = np.zeros((2 * ex, ex))
    low_x[:ex, :hx] = (level_matrix(hx) @ wx[:hx]).T
    low_x[ex:, hx:] = wx[hx:].T
    return [
        split_np(low_x),
        split_np(wx.T),
        split_np(along_y),
        split_np(along_y.T),
        split_np(low_x.T),
        split_np(wx),
    ]


def split(value):
    high = value.astype(jnp.bfloat16)
    low = (value - high.astype(jnp.float32)).astype(jnp.bfloat16)
    return high, low


def dot3(a, b):
    dot = functools.partial(jnp.dot, preferred_element_type=jnp.float32)
    return dot(a[0], b[0]) + (dot(a[0], b[1]) + dot(a[1], b[0]))


def kernel(
    sizes,
    img_hbm, grad_hbm, dual_hbm, rw_hbm, lowx_hbm, wxt_hbm, ay_hbm, ayt_hbm, lowxt_hbm, wx_hbm,
    image_next, updated, factor,
    img, grad, dual, rw, lowx, wxt, ay, ayt, lowxt, wx,
    work, fy1_s, fy1_r, fx1_s, fx1_r, fx2_s, fx2_r, fy2_s, fy2_r, total, other,
    dual_sem, img_sem, grad_sem, const_sem,
    fy1_ss, fy1_rs, fx1_ss, fx1_rs, fx2_ss, fx2_rs, fy2_ss, fy2_rs, ch_ss, ch_rs,
):
    n_fx, n_fy, chunks, tx, ty, border = sizes
    ex = tx + border
    tail = ty - LANES
    fx, fy, ch = lax.axis_index("fx"), lax.axis_index("fy"), lax.axis_index("ch")
    has_left, has_right = fx > 0, fx < n_fx - 1
    has_up, has_down = fy > 0, fy < n_fy - 1

    barrier = pltpu.get_barrier_semaphore()

    def greet(condition, where):
        @pl.when(condition)
        def _():
            pl.semaphore_signal(barrier, inc=1, device_id=where, device_id_type=MESH)

    greet(has_left, {"fx": fx - 1})
    greet(has_right, {"fx": fx + 1})
    greet(has_up, {"fy": fy - 1})
    greet(has_down, {"fy": fy + 1})
    pl.semaphore_signal(barrier, inc=1, device_id={"ch": 1 - ch}, device_id_type=MESH)

    def rows_of(k):
        return pl.ds(k * GROUP, GROUP)

    def load(src, dst, sems, k):
        return pltpu.make_async_copy(src.at[rows_of(k)], dst.at[rows_of(k)], sems.at[k])

    constants = [
        (lowx_hbm, lowx), (wxt_hbm, wxt), (ay_hbm, ay), (ayt_hbm, ayt), (lowxt_hbm, lowxt), (wx_hbm, wx), (rw_hbm, rw)
    ]

    def constant(i):
        return pltpu.make_async_copy(constants[i][0], constants[i][1], const_sem.at[i])

    load(dual_hbm, dual, dual_sem, 0).start()
    for i in range(3):
        constant(i).start()
    for k in range(1, chunks):
        load(dual_hbm, dual, dual_sem, k).start()
    for k in range(chunks):
        load(img_hbm, img, img_sem, k).start()
        load(grad_hbm, grad, grad_sem, k).start()
    for i in range(3, len(constants)):
        constant(i).start()

    def clear(condition, ref):
        @pl.when(condition)
        def _():
            ref[...] = jnp.zeros_like(ref)

    clear(fy == n_fy - 1, fy1_r)
    clear(fx == n_fx - 1, fx1_r)
    clear(fx == 0, fx2_r)
    clear(fy == 0, fy2_r)
    total[...] = jnp.zeros_like(total)

    neighbours = (
        has_left.astype(jnp.int32) + has_right.astype(jnp.int32) + has_up.astype(jnp.int32) + has_down.astype(jnp.int32) + 1
    )
    pl.semaphore_wait(barrier, neighbours)

    def remote(src, dst, send, recv, k, where):
        return pltpu.make_async_remote_copy(
            src_ref=src.at[k], dst_ref=dst.at[k], send_sem=send.at[k], recv_sem=recv.at[k],
            device_id=where, device_id_type=MESH,
        )

    def fy1(k):
        return remote(fy1_s, fy1_r, fy1_ss, fy1_rs, k, {"fy": fy - 1})

    def fx1(k):
        return remote(fx1_s, fx1_r, fx1_ss, fx1_rs, k, {"fx": fx - 1})

    def fx2(k):
        return remote(fx2_s, fx2_r, fx2_ss, fx2_rs, k, {"fx": fx + 1})

    def fy2(k):
        return remote(fy2_s, fy2_r, fy2_ss, fy2_rs, k, {"fy": fy + 1})

    lane_e = lax.broadcasted_iota(jnp.int32, (ex, LANES), 1)
    lane_b = lax.broadcasted_iota(jnp.int32, (border, LANES), 1)
    lane_h = lax.broadcasted_iota(jnp.int32, (border // 2, LANES), 1)
    half = border // 2
    low_edge = (lane_e >= tail - border) & (lane_e < tail)

    def pack(strip0, strip1, out, k):
        for c in range(GROUP):
            out[k, c * border : (c + 1) * border, :] = strip0(c)
        tiles = [strip1(c) for c in range(GROUP)]
        for p in range(GROUP // 2):
            at = GROUP * border + p * border
            out[k, at : at + border, :] = jnp.where(lane_b < 64, tiles[2 * p], pltpu.roll(tiles[2 * p + 1], 64, 1))
        rest = jnp.zeros((half, LANES), jnp.float32)
        for c in range(GROUP):
            for part in range(2):
                to = part * 64 + c * 16
                moved = pltpu.roll(tiles[c][part * half : (part + 1) * half], (to - 64) % LANES, 1)
                rest = jnp.where((lane_h >= to) & (lane_h < to + 16), moved, rest)
        at = (GROUP + GROUP // 2) * border
        out[k, at : at + half, :] = rest

    def unpack(ref, k, c):
        first = ref[k, c * border : (c + 1) * border, :]
        at = GROUP * border + (c // 2) * border
        second = ref[k, at : at + border, :]
        if c % 2:
            second = pltpu.roll(second, 64, 1)
        at = (GROUP + GROUP // 2) * border
        rest = ref[k, at : at + half, :]
        parts = []
        for part in range(2):
            shift = (64 - part * 64 - c * 16) % LANES
            parts.append(pltpu.roll(rest, shift, 1) if shift else rest)
        return first, jnp.where(lane_b < 64, second, jnp.concatenate(parts, axis=0))

    def synthesize(k):
        load(dual_hbm, dual, dual_sem, k).wait()
        mat_low, mat_x, mat_y = [(m[0], m[1]) for m in (lowx, wxt, ay)]
        for p in range(GROUP // 2):
            a, b = k * GROUP + 2 * p, k * GROUP + 2 * p + 1
            left = jnp.concatenate([dual[a, :, :LANES], dual[b, :, :LANES]], axis=1)
            right = jnp.concatenate([dual[a, :, LANES:], dual[b, :, LANES:]], axis=1)
            from_left = dot3(mat_low, split(left))
            from_right = dot3(mat_x, split(right))
            tiles = []
            for c, at in ((a, 0), (b, LANES)):
                lanes = slice(at, at + LANES)
                rows = jnp.concatenate([from_left[:ex, lanes], from_left[ex:, lanes], from_right[:, lanes]], axis=1)
                result = dot3(split(rows), mat_y)
                work[c] = result
                tiles.append(result[:, LANES:])
            fy1_s[k, p] = jnp.where(
                low_edge, pltpu.roll(tiles[0], LANES - border, 1), pltpu.roll(tiles[1], 64 - border, 1)
            )
        pl.when(has_up)(lambda: fy1(k).start())

    def send_columns(k):
        pl.when(has_down)(lambda: fy1(k).wait_recv())
        for p in range(GROUP // 2):
            a, b = k * GROUP + 2 * p, k * GROUP + 2 * p + 1
            strip = fy1_r[k, p]
            work[a, :, LANES:] = work[a, :, LANES:] + jnp.where(low_edge, strip, 0.0)
            work[b, :, LANES:] = work[b, :, LANES:] + jnp.where(low_edge, pltpu.roll(strip, 64, 1), 0.0)

        pack(
            lambda c: work[k * GROUP + c, :border, :LANES],
            lambda c: work[k * GROUP + c, :border, LANES:],
            fx1_s, k,
        )
        pl.when(has_left)(lambda: fx1(k).start())

    root = jnp.float32(0.5**0.5)

    def weights(lane_from):
        rows = lax.broadcasted_iota(jnp.int32, (tx, LANES), 0)
        lanes = lax.broadcasted_iota(jnp.int32, (tx, LANES), 1) + lane_from
        by_x = jnp.where((rows >= tx - border) & has_right, root, 1.0)
        by_y = jnp.where((lanes >= ty - border) & has_down, root, 1.0)
        return by_x * by_y

    def update_image(k):
        load(img_hbm, img, img_sem, k).wait()
        load(grad_hbm, grad, grad_sem, k).wait()
        pl.when(has_right)(lambda: fx1(k).wait_recv())
        w0 = weights(0)
        w1 = weights(LANES)[:, :tail]
        for c in range(GROUP):
            i = k * GROUP + c
            add0, add1 = unpack(fx1_r, k, c)
            for own, add, w, lanes in (
                (work[i, border:, :LANES], add0, w0, slice(0, LANES)),
                (work[i, border:, LANES : LANES + tail], add1[:, :tail], w1, slice(LANES, LANES + tail)),
            ):
                keep = tx - border
                summed = jnp.concatenate([own[:keep], own[keep:] + add], axis=0)
                image = img[i, :, lanes]
                step = jnp.maximum(image - TAU_STEP * (grad[i, :, lanes].astype(jnp.float32) + summed * w), 0.0)
                extrap = (2.0 * step - image) * w
                image_next[i, :, lanes] = step
                work[i, border:, lanes] = extrap
        pack(
            lambda c: work[k * GROUP + c, tx:, :LANES],
            lambda c: work[k * GROUP + c, tx:, LANES:],
            fx2_s, k,
        )
        pl.when(has_right)(lambda: fx2(k).start())

    def send_rows(k):
        pl.when(has_left)(lambda: fx2(k).wait_recv())
        for p in range(GROUP // 2):
            tiles = []
            for c in (2 * p, 2 * p + 1):
                i = k * GROUP + c
                add0, add1 = unpack(fx2_r, k, c)
                work[i, :border, :LANES] = add0
                work[i, :border, LANES:] = add1
                tiles.append(jnp.concatenate([add1, work[i, border:, LANES:]], axis=0))
            fy2_s[k, p] = jnp.where(lane_e >= tail, pltpu.roll(tiles[0], border, 1), pltpu.roll(tiles[1], 64 + border, 1))
        pl.when(has_down)(lambda: fy2(k).start())

    def analyse(k):
        pl.when(has_up)(lambda: fy2(k).wait_recv())
        mat_y, mat_low, mat_x = [(m[0], m[1]) for m in (ayt, lowxt, wx)]
        for p in range(GROUP // 2):
            a, b = k * GROUP + 2 * p, k * GROUP + 2 * p + 1
            strip = fy2_r[k, p]
            results = []
            for i, moved in ((a, strip), (b, pltpu.roll(strip, 64, 1))):
                second = jnp.where(lane_e < tail, work[i, :, LANES:], moved)
                window = jnp.concatenate([work[i, :, :LANES], second], axis=1)
                results.append(dot3(split(window), mat_y))
            va, vb = results
            left = jnp.concatenate(
                [
                    jnp.concatenate([va[:, :LANES], vb[:, :LANES]], axis=1),
                    jnp.concatenate([va[:, LANES : 2 * LANES], vb[:, LANES : 2 * LANES]], axis=1),
                ],
                axis=0,
            )
            right = jnp.concatenate([va[:, 2 * LANES :], vb[:, 2 * LANES :]], axis=1)
            low = dot3(mat_low, split(left))
            high = dot3(mat_x, split(right))
            for lanes, part in ((slice(0, LANES), low), (slice(LANES, 2 * LANES), high)):
                first = dual[a, :, lanes] + part[:, :LANES]
                second = dual[b, :, lanes] + part[:, LANES:]
                updated[a, :, lanes] = first
                updated[b, :, lanes] = second
                total[:, lanes] = total[:, lanes] + (first * first + second * second)

    for i in range(len(constants)):
        constant(i).wait()

    phases = ((synthesize, 0), (send_columns, 1), (update_image, 3), (send_rows, 5), (analyse, 6))

    def step(s, carry):
        for phase, lag in phases:

            @pl.when((s >= lag) & (s < chunks + lag))
            def _(phase=phase, lag=lag):
                phase(s - lag)

        return carry

    lax.fori_loop(0, chunks + phases[-1][1], step, 0)

    swap = pltpu.make_async_remote_copy(
        src_ref=total, dst_ref=other, send_sem=ch_ss, recv_sem=ch_rs, device_id={"ch": 1 - ch}, device_id_type=MESH
    )
    swap.start()

    def drain(k, carry):
        pl.when(has_up)(lambda: fy1(k).wait_send())
        pl.when(has_left)(lambda: fx1(k).wait_send())
        pl.when(has_right)(lambda: fx2(k).wait_send())
        pl.when(has_down)(lambda: fy2(k).wait_send())
        return carry

    lax.fori_loop(0, chunks, drain, 0)
    swap.wait()
    factor[...] = jnp.minimum(1.0, LAMBDA_REG * rw[...] / jnp.sqrt(total[...] + other[...] + EPSILON))


def shards(mesh_shape, image_cube, data_grad, dual_coeffs, reweights):
    channels, tx, ty = image_cube.shape
    _, ex, ey = dual_coeffs.shape
    border = ex - tx
    chunks = channels // GROUP
    constants = [jnp.asarray(m) for m in matrices(ex, ey, border)]
    sizes = (mesh_shape["fx"], mesh_shape["fy"], chunks, tx, ty, border)
    f32 = jnp.float32
    strip_y = (chunks, GROUP // 2, ex, LANES)
    strip_x = (chunks, GROUP * border * ty // LANES, LANES)
    dma = pltpu.SemaphoreType.DMA
    in_hbm = pl.BlockSpec(memory_space=pltpu.HBM)
    in_vmem = pl.BlockSpec(memory_space=pltpu.VMEM)
    image_next, updated, factor = pl.pallas_call(
        functools.partial(kernel, sizes),
        out_shape=(
            jax.ShapeDtypeStruct(image_cube.shape, f32),
            jax.ShapeDtypeStruct(dual_coeffs.shape, f32),
            jax.ShapeDtypeStruct(reweights.shape, f32),
        ),
        in_specs=[in_hbm] * (4 + len(constants)),
        out_specs=(in_vmem,) * 3,
        scratch_shapes=[
            pltpu.VMEM(image_cube.shape, f32),
            pltpu.VMEM(data_grad.shape, data_grad.dtype),
            pltpu.VMEM(dual_coeffs.shape, f32),
            pltpu.VMEM(reweights.shape, f32),
            *[pltpu.VMEM(m.shape, m.dtype) for m in constants],
            pltpu.VMEM(dual_coeffs.shape, f32),
            pltpu.VMEM(strip_y, f32), pltpu.VMEM(strip_y, f32),
            pltpu.VMEM(strip_x, f32), pltpu.VMEM(strip_x, f32),
            pltpu.VMEM(strip_x, f32), pltpu.VMEM(strip_x, f32),
            pltpu.VMEM(strip_y, f32), pltpu.VMEM(strip_y, f32),
            pltpu.VMEM((ex, ey), f32), pltpu.VMEM((ex, ey), f32),
            dma((chunks,)), dma((chunks,)), dma((chunks,)), dma((7,)),
            *[dma((chunks,)) for _ in range(8)],
            dma, dma,
        ],
        compiler_params=pltpu.CompilerParams(
            collective_id=0, has_side_effects=True, vmem_limit_bytes=40 * 2**20
        ),
        name="primal_dual",
    )(*[pltpu.with_memory_space_constraint(x, pltpu.HBM) for x in (image_cube, data_grad, dual_coeffs, reweights, *constants)])
    return image_next, updated * factor[None]


def solution(mesh):
    return jax.shard_map(
        functools.partial(shards, dict(mesh.shape)),
        mesh=mesh,
        in_specs=(P("ch", "fx", "fy"), P("ch", "fx", "fy"), P("ch", "fx", "fy"), P("fx", "fy")),
        out_specs=(P("ch", "fx", "fy"), P("ch", "fx", "fy")),
        check_vma=False,
    )
```

```python
import functools

import jax
import jax.numpy as jnp
import numpy as np
from jax import lax
from jax.experimental import pallas as pl
from jax.experimental.pallas import tpu as pltpu
from jax.sharding import PartitionSpec as P

LOW_PASS = [
    -0.00011747678400228192,
    0.0006754494059985568,
    -0.0003917403729959771,
    -0.00487035299301066,
    0.008746094047015655,
    0.013981027917015516,
    -0.04408825393106472,
    -0.01736930100202211,
    0.128747426620186,
    0.00047248457399797254,
    -0.2840155429624281,
    -0.015829105256023893,
    0.5853546836548691,
    0.6756307362980128,
    0.3128715909144659,
    0.05441584224308161,
]
TAU_STEP = 0.5
LAMBDA_REG = 1.0
EPSILON = 1e-06
LANES = 128
GROUP = 4
MESH = pl.DeviceIdType.MESH


def level_matrix(length):
    halved = length // 2
    taps_count = len(LOW_PASS)
    matrix = np.zeros((length, length))
    for out_row in range(halved):
        for tap_index in range(taps_count):
            column = (2 * out_row + tap_index) % length
            matrix[out_row, column] += LOW_PASS[tap_index]
            matrix[halved + out_row, column] += (-1) ** tap_index * LOW_PASS[
                taps_count - 1 - tap_index
            ]
    return matrix


def split_np(matrix):
    single = matrix.astype(np.float32)
    high = single.astype(jnp.bfloat16)
    low = (single - high.astype(np.float32)).astype(jnp.bfloat16)
    return np.stack([high, low])


def matrices(ex, ey, border):
    wx, wy = level_matrix(ex), level_matrix(ey)
    hx, hy = ex // 2, ey // 2
    along_y = np.concatenate([level_matrix(hy) @ wy[:hy], wy], axis=0)
    order = np.concatenate([np.arange(border, ey), np.arange(border)])
    along_y = along_y[:, order]
    low_x = np.zeros((2 * ex, ex))
    low_x[:ex, :hx] = (level_matrix(hx) @ wx[:hx]).T
    low_x[ex:, hx:] = wx[hx:].T
    return [
        split_np(low_x),
        split_np(wx.T),
        split_np(along_y),
        split_np(along_y.T),
        split_np(low_x.T),
        split_np(wx),
    ]


def split(value):
    high = value.astype(jnp.bfloat16)
    low = (value - high.astype(jnp.float32)).astype(jnp.bfloat16)
    return high, low


def dot3(a, b):
    dot = functools.partial(jnp.dot, preferred_element_type=jnp.float32)
    return dot(a[0], b[0]) + (dot(a[0], b[1]) + dot(a[1], b[0]))


def kernel(
    sizes,
    img_hbm, grad_hbm, dual_hbm, rw_hbm, lowx_hbm, wxt_hbm, ay_hbm, ayt_hbm, lowxt_hbm, wx_hbm,
    image_next, updated, factor,
    img, grad, dual, rw, lowx, wxt, ay, ayt, lowxt, wx,
    work, rows_hi, rows_lo, mixed,
    fy1_s, fy1_r, bulk1_s, bulk1_r, corner1_s, corner1_r,
    bulk2_s, bulk2_r, corner2_s, corner2_r, fy2_s, fy2_r, total, other,
    dual_sem, img_sem, grad_sem, const_sem,
    fy1_ss, fy1_rs, bulk1_ss, bulk1_rs, corner1_ss, corner1_rs,
    bulk2_ss, bulk2_rs, corner2_ss, corner2_rs, fy2_ss, fy2_rs, ch_ss, ch_rs,
):
    n_fx, n_fy, chunks, tx, ty, border = sizes
    ex = tx + border
    ey = ty + border
    tail = ty - LANES
    half = border // 2
    fx, fy, ch = lax.axis_index("fx"), lax.axis_index("fy"), lax.axis_index("ch")
    has_left, has_right = fx > 0, fx < n_fx - 1
    has_up, has_down = fy > 0, fy < n_fy - 1

    barrier = pltpu.get_barrier_semaphore()

    def greet(condition, where):
        @pl.when(condition)
        def _():
            pl.semaphore_signal(barrier, inc=1, device_id=where, device_id_type=MESH)

    greet(has_left, {"fx": fx - 1})
    greet(has_right, {"fx": fx + 1})
    greet(has_up, {"fy": fy - 1})
    greet(has_down, {"fy": fy + 1})
    pl.semaphore_signal(barrier, inc=1, device_id={"ch": 1 - ch}, device_id_type=MESH)
    neighbours = 1 + sum(c.astype(jnp.int32) for c in (has_left, has_right, has_up, has_down))

    def load(src, dst, sems, k):
        rows = pl.ds(k * GROUP, GROUP)
        return pltpu.make_async_copy(src.at[rows], dst.at[rows], sems.at[k])

    constants = [
        (lowx_hbm, lowx), (wxt_hbm, wxt), (ay_hbm, ay), (ayt_hbm, ayt), (lowxt_hbm, lowxt), (wx_hbm, wx), (rw_hbm, rw)
    ]

    def constant(i):
        return pltpu.make_async_copy(constants[i][0], constants[i][1], const_sem.at[i])

    load(dual_hbm, dual, dual_sem, 0).start()
    for i in range(3):
        constant(i).start()
    for k in range(1, chunks):
        load(dual_hbm, dual, dual_sem, k).start()
    for k in range(chunks):
        load(img_hbm, img, img_sem, k).start()
        load(grad_hbm, grad, grad_sem, k).start()
    for i in range(3, len(constants)):
        constant(i).start()

    def clear(condition, *refs):
        @pl.when(condition)
        def _():
            for ref in refs:
                ref[...] = jnp.zeros_like(ref)

    clear(fy == n_fy - 1, fy1_r)
    clear(fx == n_fx - 1, bulk1_r, corner1_r)
    clear(fx == 0, bulk2_r, corner2_r)
    clear(fy == 0, fy2_r)
    total[...] = jnp.zeros_like(total)

    def remote(src, dst, send, recv, k, where):
        return pltpu.make_async_remote_copy(
            src_ref=src.at[k], dst_ref=dst.at[k], send_sem=send.at[k], recv_sem=recv.at[k],
            device_id=where, device_id_type=MESH,
        )

    def fy1(k):
        return remote(fy1_s, fy1_r, fy1_ss, fy1_rs, k, {"fy": fy - 1})

    def bulk1(k):
        return remote(bulk1_s, bulk1_r, bulk1_ss, bulk1_rs, k, {"fx": fx - 1})

    def corner1(k):
        return remote(corner1_s, corner1_r, corner1_ss, corner1_rs, k, {"fx": fx - 1})

    def bulk2(k):
        return remote(bulk2_s, bulk2_r, bulk2_ss, bulk2_rs, k, {"fx": fx + 1})

    def corner2(k):
        return remote(corner2_s, corner2_r, corner2_ss, corner2_rs, k, {"fx": fx + 1})

    def fy2(k):
        return remote(fy2_s, fy2_r, fy2_ss, fy2_rs, k, {"fy": fy + 1})

    lane_e = lax.broadcasted_iota(jnp.int32, (ex, LANES), 1)
    lane_b = lax.broadcasted_iota(jnp.int32, (border, LANES), 1)
    lane_h = lax.broadcasted_iota(jnp.int32, (half, LANES), 1)
    low_edge = (lane_e >= tail - border) & (lane_e < tail)

    def roll(value, shift):
        shift = shift % LANES
        return pltpu.roll(value, shift, 1) if shift else value

    def pack_bulk(tile0, tile1, out, k):
        joined = jnp.zeros((border, LANES), jnp.float32)
        for c in range(GROUP):
            out[k, c * border : (c + 1) * border, :] = tile0(c)
            moved = roll(tile1(c), 32 * c)
            joined = jnp.where((lane_b >= 32 * c) & (lane_b < 32 * c + 32), moved, joined)
        out[k, GROUP * border : (GROUP + 1) * border, :] = joined

    def pack_corner(tile1, out, k):
        joined = jnp.zeros((border, LANES), jnp.float32)
        rest = jnp.zeros((half, LANES), jnp.float32)
        for c in range(GROUP):
            value = tile1(c)
            moved = roll(value, 32 * c - 32)
            joined = jnp.where((lane_b >= 32 * c) & (lane_b < 32 * c + 32), moved, joined)
            for part in range(2):
                to = part * 64 + c * 16
                moved = roll(value[part * half : (part + 1) * half], to - 64)
                rest = jnp.where((lane_h >= to) & (lane_h < to + 16), moved, rest)
        out[k, :border, :] = joined
        out[k, border:, :] = rest

    def unpack_corner(ref, k, c):
        middle = roll(ref[k, :border, :], 32 - 32 * c)
        parts = [roll(ref[k, border:, :], 64 - part * 64 - c * 16) for part in range(2)]
        return jnp.where(lane_b < 64, middle, jnp.concatenate(parts, axis=0))

    def unpack(bulk, corner, k, c):
        first = bulk[k, c * border : (c + 1) * border, :]
        start = roll(bulk[k, GROUP * border : (GROUP + 1) * border, :], -32 * c)
        return first, jnp.where(lane_b < 32, start, unpack_corner(corner, k, c))

    def put_rows(at, lanes, value):
        high = value.astype(jnp.bfloat16)
        rows_hi[at : at + ex, lanes] = high
        rows_lo[at : at + ex, lanes] = (value - high.astype(jnp.float32)).astype(jnp.bfloat16)

    def synthesize(k):
        load(dual_hbm, dual, dual_sem, k).wait()
        first = k * GROUP
        left = jnp.concatenate([dual[first + c, :, :LANES] for c in range(GROUP)], axis=1)
        from_left = dot3((lowx[0], lowx[1]), split(left))
        for c in range(GROUP):
            lanes = slice(c * LANES, (c + 1) * LANES)
            put_rows(c * ex, slice(0, LANES), from_left[:ex, lanes])
            put_rows(c * ex, slice(LANES, 2 * LANES), from_left[ex:, lanes])
        right = jnp.concatenate([dual[first + c, :, LANES:] for c in range(GROUP)], axis=1)
        from_right = dot3((wxt[0], wxt[1]), split(right))
        for c in range(GROUP):
            put_rows(c * ex, slice(2 * LANES, 3 * LANES), from_right[:, c * LANES : (c + 1) * LANES])
        result = dot3((rows_hi[...], rows_lo[...]), (ay[0], ay[1]))
        for c in range(GROUP):
            work[first + c] = result[c * ex : (c + 1) * ex]

        @pl.when(k == 0)
        def _():
            pl.semaphore_wait(barrier, neighbours)

        for p in range(GROUP // 2):
            a, b = work[first + 2 * p, :, LANES:], work[first + 2 * p + 1, :, LANES:]
            fy1_s[k, p] = jnp.where(low_edge, roll(a, -border), roll(b, 64 - border))
        pl.when(has_up)(lambda: fy1(k).start())
        pack_bulk(
            lambda c: work[first + c, :border, :LANES], lambda c: work[first + c, :border, LANES:], bulk1_s, k
        )
        pl.when(has_left)(lambda: bulk1(k).start())

    def send_columns(k):
        pl.when(has_down)(lambda: fy1(k).wait_recv())
        for p in range(GROUP // 2):
            a = k * GROUP + 2 * p
            strip = fy1_r[k, p]
            work[a, :, LANES:] = work[a, :, LANES:] + jnp.where(low_edge, strip, 0.0)
            work[a + 1, :, LANES:] = work[a + 1, :, LANES:] + jnp.where(low_edge, roll(strip, 64), 0.0)
        pack_corner(lambda c: work[k * GROUP + c, :border, LANES:], corner1_s, k)
        pl.when(has_left)(lambda: corner1(k).start())

    root = jnp.float32(0.5**0.5)

    def weights(lane_from):
        rows = lax.broadcasted_iota(jnp.int32, (tx, LANES), 0)
        lanes = lax.broadcasted_iota(jnp.int32, (tx, LANES), 1) + lane_from
        by_x = jnp.where((rows >= tx - border) & has_right, root, 1.0)
        by_y = jnp.where((lanes >= ty - border) & has_down, root, 1.0)
        return by_x * by_y

    def update_image(k):
        load(img_hbm, img, img_sem, k).wait()
        load(grad_hbm, grad, grad_sem, k).wait()

        @pl.when(has_right)
        def _():
            bulk1(k).wait_recv()
            corner1(k).wait_recv()

        keep = tx - border
        w0 = weights(0)
        w1 = weights(LANES)[:, :tail]
        for c in range(GROUP):
            i = k * GROUP + c
            add0, add1 = unpack(bulk1_r, corner1_r, k, c)
            for own, add, w, lanes in (
                (work[i, border:, :LANES], add0, w0, slice(0, LANES)),
                (work[i, border:, LANES:ty], add1[:, :tail], w1, slice(LANES, ty)),
            ):
                summed = jnp.concatenate([own[:keep], own[keep:] + add], axis=0)
                image = img[i, :, lanes]
                step = jnp.maximum(image - TAU_STEP * (grad[i, :, lanes].astype(jnp.float32) + summed * w), 0.0)
                image_next[i, :, lanes] = step
                work[i, border:, lanes] = (2.0 * step - image) * w
        pack_corner(lambda c: work[k * GROUP + c, tx:, LANES:], corner2_s, k)
        pl.when(has_right)(lambda: corner2(k).start())
        pack_bulk(
            lambda c: work[k * GROUP + c, tx:, :LANES], lambda c: work[k * GROUP + c, tx:, LANES:], bulk2_s, k
        )
        pl.when(has_right)(lambda: bulk2(k).start())

    def send_rows(k):
        pl.when(has_left)(lambda: corner2(k).wait_recv())
        for p in range(GROUP // 2):
            a, b = [
                jnp.concatenate([unpack_corner(corner2_r, k, c), work[k * GROUP + c, border:, LANES:]], axis=0)
                for c in (2 * p, 2 * p + 1)
            ]
            fy2_s[k, p] = jnp.where(lane_e >= tail, roll(a, border), roll(b, 64 + border))
        pl.when(has_down)(lambda: fy2(k).start())

    def analyse(k):
        @pl.when(k == 0)
        def _():
            for i in range(3, len(constants)):
                constant(i).wait()

        pl.when(has_left)(lambda: bulk2(k).wait_recv())
        pl.when(has_up)(lambda: fy2(k).wait_recv())
        first = k * GROUP
        for c in range(GROUP):
            i = first + c
            strip = roll(fy2_r[k, c // 2], 64 * (c % 2))
            edge0, edge1 = unpack(bulk2_r, corner2_r, k, c)
            put_rows(c * ex, slice(0, LANES), jnp.concatenate([edge0, work[i, border:, :LANES]], axis=0))
            second = jnp.concatenate([edge1, work[i, border:, LANES:]], axis=0)
            put_rows(c * ex, slice(LANES, 2 * LANES), jnp.where(lane_e < tail, second, strip))
        mixed[...] = dot3((rows_hi[:, :ey], rows_lo[:, :ey]), (ayt[0], ayt[1]))

        def beside(tile):
            lanes = slice(tile * LANES, (tile + 1) * LANES)
            return jnp.concatenate([mixed[c * ex : (c + 1) * ex, lanes] for c in range(GROUP)], axis=1)

        low = dot3((lowxt[0], lowxt[1]), split(jnp.concatenate([beside(0), beside(1)], axis=0)))
        high = dot3((wx[0], wx[1]), split(beside(2)))
        for lanes, part in ((slice(0, LANES), low), (slice(LANES, 2 * LANES), high)):
            squares = total[:, lanes]
            for c in range(GROUP):
                value = dual[first + c, :, lanes] + part[:, c * LANES : (c + 1) * LANES]
                updated[first + c, :, lanes] = value
                squares = squares + value * value
            total[:, lanes] = squares

    for i in range(3):
        constant(i).wait()

    phases = ((synthesize, 0), (send_columns, 1), (update_image, 3), (send_rows, 5), (analyse, 6))

    def step(s, carry):
        for phase, lag in phases:

            @pl.when((s >= lag) & (s < chunks + lag))
            def _(phase=phase, lag=lag):
                phase(s - lag)

        return carry

    lax.fori_loop(0, chunks + phases[-1][1], step, 0)

    swap = pltpu.make_async_remote_copy(
        src_ref=total, dst_ref=other, send_sem=ch_ss, recv_sem=ch_rs, device_id={"ch": 1 - ch}, device_id_type=MESH
    )
    swap.start()

    def drain(k, carry):
        pl.when(has_up)(lambda: fy1(k).wait_send())

        @pl.when(has_left)
        def _():
            bulk1(k).wait_send()
            corner1(k).wait_send()

        @pl.when(has_right)
        def _():
            bulk2(k).wait_send()
            corner2(k).wait_send()

        pl.when(has_down)(lambda: fy2(k).wait_send())
        return carry

    lax.fori_loop(0, chunks, drain, 0)
    swap.wait()
    factor[...] = jnp.minimum(1.0, LAMBDA_REG * rw[...] / jnp.sqrt(total[...] + other[...] + EPSILON))


def finish(chunks, image, updated, factor, image_out, dual_out, scaled, image_sem, sems):
    pltpu.make_async_copy(image, image_out, image_sem).start()

    def copy(k):
        rows = pl.ds(k * GROUP, GROUP)
        return pltpu.make_async_copy(scaled.at[rows], dual_out.at[rows], sems.at[k])

    def step(k, carry):
        for c in range(GROUP):
            scaled[k * GROUP + c] = updated[k * GROUP + c] * factor[...]
        copy(k).start()
        return carry

    lax.fori_loop(0, chunks, step, 0)
    pltpu.make_async_copy(image, image_out, image_sem).wait()

    def drain(k, carry):
        copy(k).wait()
        return carry

    lax.fori_loop(0, chunks, drain, 0)


def shards(mesh_shape, image_cube, data_grad, dual_coeffs, reweights):
    channels, tx, ty = image_cube.shape
    _, ex, ey = dual_coeffs.shape
    border = ex - tx
    chunks = channels // GROUP
    constants = [jnp.asarray(m) for m in matrices(ex, ey, border)]
    sizes = (mesh_shape["fx"], mesh_shape["fy"], chunks, tx, ty, border)
    f32, bf16 = jnp.float32, jnp.bfloat16
    strip_y = pltpu.VMEM((chunks, GROUP // 2, ex, LANES), f32)
    bulk = pltpu.VMEM((chunks, (GROUP + 1) * border, LANES), f32)
    corner = pltpu.VMEM((chunks, border + border // 2, LANES), f32)
    dma = pltpu.SemaphoreType.DMA
    in_hbm = pl.BlockSpec(memory_space=pltpu.HBM)
    in_vmem = pl.BlockSpec(memory_space=pltpu.VMEM)
    operands = [
        pltpu.with_memory_space_constraint(x, pltpu.HBM)
        for x in (image_cube, data_grad, dual_coeffs, reweights, *constants)
    ]
    image_next, updated, factor = pl.pallas_call(
        functools.partial(kernel, sizes),
        out_shape=(
            jax.ShapeDtypeStruct(image_cube.shape, f32),
            jax.ShapeDtypeStruct(dual_coeffs.shape, f32),
            jax.ShapeDtypeStruct(reweights.shape, f32),
        ),
        in_specs=[in_hbm] * len(operands),
        out_specs=(in_vmem,) * 3,
        scratch_shapes=[
            pltpu.VMEM(image_cube.shape, f32),
            pltpu.VMEM(data_grad.shape, data_grad.dtype),
            pltpu.VMEM(dual_coeffs.shape, f32),
            pltpu.VMEM(reweights.shape, f32),
            *[pltpu.VMEM(m.shape, m.dtype) for m in constants],
            pltpu.VMEM(dual_coeffs.shape, f32),
            pltpu.VMEM((GROUP * ex, ey + LANES), bf16),
            pltpu.VMEM((GROUP * ex, ey + LANES), bf16),
            pltpu.VMEM((GROUP * ex, ey + LANES), f32),
            strip_y, strip_y, bulk, bulk, corner, corner, bulk, bulk, corner, corner, strip_y, strip_y,
            pltpu.VMEM((ex, ey), f32), pltpu.VMEM((ex, ey), f32),
            dma((chunks,)), dma((chunks,)), dma((chunks,)), dma((7,)),
            *[dma((chunks,)) for _ in range(12)],
            dma, dma,
        ],
        compiler_params=pltpu.CompilerParams(
            collective_id=0, has_side_effects=True, vmem_limit_bytes=40 * 2**20
        ),
        name="primal_dual",
    )(*operands)
    return pl.pallas_call(
        functools.partial(finish, chunks),
        out_shape=(
            jax.ShapeDtypeStruct(image_cube.shape, f32),
            jax.ShapeDtypeStruct(dual_coeffs.shape, f32),
        ),
        in_specs=[in_vmem] * 3,
        out_specs=(in_hbm,) * 2,
        scratch_shapes=[pltpu.VMEM(dual_coeffs.shape, f32), dma, dma((chunks,))],
        compiler_params=pltpu.CompilerParams(vmem_limit_bytes=16 * 2**20),
        name="scaled_results",
    )(image_next, updated, factor)


def solution(mesh):
    return jax.shard_map(
        functools.partial(shards, dict(mesh.shape)),
        mesh=mesh,
        in_specs=(P("ch", "fx", "fy"), P("ch", "fx", "fy"), P("ch", "fx", "fy"), P("fx", "fy")),
        out_specs=(P("ch", "fx", "fy"), P("ch", "fx", "fy")),
        check_vma=False,
    )
```

```python
import functools

import jax
import jax.numpy as jnp
import numpy as np
from jax import lax
from jax.experimental import pallas as pl
from jax.experimental.pallas import tpu as pltpu
from jax.sharding import PartitionSpec as P

LOW_PASS = [
    -0.00011747678400228192,
    0.0006754494059985568,
    -0.0003917403729959771,
    -0.00487035299301066,
    0.008746094047015655,
    0.013981027917015516,
    -0.04408825393106472,
    -0.01736930100202211,
    0.128747426620186,
    0.00047248457399797254,
    -0.2840155429624281,
    -0.015829105256023893,
    0.5853546836548691,
    0.6756307362980128,
    0.3128715909144659,
    0.05441584224308161,
]
TAU_STEP = 0.5
LAMBDA_REG = 1.0
EPSILON = 1e-06
LANES = 128
GROUP = 4
RUN = 4
RELAYED_LEFT = ((0, 1, 3, 4, 6), (1, 3, 5), (3,))
RELAYED_RIGHT = ((2, 6), (0, 2, 4, 6), (0, 1, 2, 4, 5, 6))
IMAGE_LAG = (5, 8)
ROWS_LAG = (13, 16)
RELAY_LAG = (3, 7)
MESH = pl.DeviceIdType.MESH


def level_matrix(length):
    halved = length // 2
    taps_count = len(LOW_PASS)
    matrix = np.zeros((length, length))
    for out_row in range(halved):
        for tap_index in range(taps_count):
            column = (2 * out_row + tap_index) % length
            matrix[out_row, column] += LOW_PASS[tap_index]
            matrix[halved + out_row, column] += (-1) ** tap_index * LOW_PASS[
                taps_count - 1 - tap_index
            ]
    return matrix


def split_np(matrix):
    single = matrix.astype(np.float32)
    high = single.astype(jnp.bfloat16)
    low = (single - high.astype(np.float32)).astype(jnp.bfloat16)
    return np.stack([high, low])


def matrices(ex, ey, border):
    wx, wy = level_matrix(ex), level_matrix(ey)
    hx, hy = ex // 2, ey // 2
    along_y = np.concatenate([level_matrix(hy) @ wy[:hy], wy], axis=0)
    order = np.concatenate([np.arange(border, ey), np.arange(border)])
    along_y = along_y[:, order]
    low_x = np.zeros((2 * ex, ex))
    low_x[:ex, :hx] = (level_matrix(hx) @ wx[:hx]).T
    low_x[ex:, hx:] = wx[hx:].T
    return [
        split_np(low_x),
        split_np(wx.T),
        split_np(along_y),
        split_np(along_y.T),
        split_np(low_x.T),
        split_np(wx),
    ]


def split(value):
    high = value.astype(jnp.bfloat16)
    low = (value - high.astype(jnp.float32)).astype(jnp.bfloat16)
    return high, low


def dot3(a, b):
    dot = functools.partial(jnp.dot, preferred_element_type=jnp.float32)
    return dot(a[0], b[0]) + (dot(a[0], b[1]) + dot(a[1], b[0]))


def kernel(
    sizes,
    img_hbm, grad_hbm, dual_hbm, rw_hbm, lowx_hbm, wxt_hbm, ay_hbm, ayt_hbm, lowxt_hbm, wx_hbm,
    image_next, updated, factor,
    img, grad, dual, rw, lowx, wxt, ay, ayt, lowxt, wx,
    work, rows_hi, rows_lo, mixed,
    fy1_s, fy1_r, bulk1_s, bulk1_r, corner1_s, corner1_r,
    bulk2_s, bulk2_r, corner2_s, corner2_r, fy2_s, fy2_r, via_bulk, via_corner, total, other,
    dual_sem, img_sem, grad_sem, const_sem,
    fy1_ss, fy1_rs, bulk1_ss, bulk1_rs, corner1_ss, corner1_rs,
    bulk2_ss, bulk2_rs, corner2_ss, corner2_rs, fy2_ss, fy2_rs,
    via_bulk_ss, via_bulk_rs, via_corner_ss, via_corner_rs, ch_ss, ch_rs,
):
    n_fx, n_fy, chunks, tx, ty, border = sizes
    ex = tx + border
    ey = ty + border
    tail = ty - LANES
    half = border // 2
    fx, fy, ch = lax.axis_index("fx"), lax.axis_index("fy"), lax.axis_index("ch")
    has_left, has_right = fx > 0, fx < n_fx - 1
    has_up, has_down = fy > 0, fy < n_fy - 1

    relays = n_fx == RUN * RUN
    run, place = fx // RUN, fx % RUN
    at_first, at_last = place == 0, place == RUN - 1
    if relays:
        crosses_left, crosses_right = at_first & has_left, at_last & has_right
        via1_here, via2_here = at_first & (run < RUN - 1), at_last & (run > 0)
    else:
        crosses_left = crosses_right = via1_here = via2_here = False

    def among(chosen, pair, k):
        found = False
        for index, listed in enumerate(chosen):
            for member in listed:
                found = found | ((pair == index) & (k == member))
        return found

    def by_relay(crosses, relayed, direct, relay, action):
        if not relays:
            return action(direct())
        pl.when(crosses & relayed)(lambda: action(relay()))
        pl.when(jnp.logical_not(crosses & relayed))(lambda: action(direct()))

    def left_relayed(k):
        return among(RELAYED_LEFT, run - 1, k)

    def right_relayed(k):
        return among(RELAYED_RIGHT, run, k)

    barrier = pltpu.get_barrier_semaphore()

    def greet(condition, where):
        @pl.when(condition)
        def _():
            pl.semaphore_signal(barrier, inc=1, device_id=where, device_id_type=MESH)

    greet(has_left, {"fx": fx - 1})
    greet(has_right, {"fx": fx + 1})
    greet(has_up, {"fy": fy - 1})
    greet(has_down, {"fy": fy + 1})
    pl.semaphore_signal(barrier, inc=1, device_id={"ch": 1 - ch}, device_id_type=MESH)
    neighbours = 1 + sum(c.astype(jnp.int32) for c in (has_left, has_right, has_up, has_down))
    if relays:
        ends = at_first | at_last
        for condition, offset in (
            (ends & (run > 0), -RUN), (ends & (run < RUN - 1), RUN), (at_first, RUN - 1), (at_last, 1 - RUN)
        ):
            greet(condition, {"fx": fx + offset})
            neighbours = neighbours + condition.astype(jnp.int32)

    def load(src, dst, sems, k):
        rows = pl.ds(k * GROUP, GROUP)
        return pltpu.make_async_copy(src.at[rows], dst.at[rows], sems.at[k])

    constants = [
        (lowx_hbm, lowx), (wxt_hbm, wxt), (ay_hbm, ay), (ayt_hbm, ayt), (lowxt_hbm, lowxt), (wx_hbm, wx), (rw_hbm, rw)
    ]

    def constant(i):
        return pltpu.make_async_copy(constants[i][0], constants[i][1], const_sem.at[i])

    load(dual_hbm, dual, dual_sem, 0).start()
    for i in range(3):
        constant(i).start()
    def clear(condition, *refs):
        @pl.when(condition)
        def _():
            for ref in refs:
                ref[...] = jnp.zeros_like(ref)

    clear(fy == n_fy - 1, fy1_r)
    clear(fx == n_fx - 1, bulk1_r, corner1_r)
    clear(fx == 0, bulk2_r, corner2_r)
    clear(fy == 0, fy2_r)
    total[...] = jnp.zeros_like(total)

    def remote(src, dst, send, recv, k, where):
        return pltpu.make_async_remote_copy(
            src_ref=src.at[k], dst_ref=dst.at[k], send_sem=send.at[k], recv_sem=recv.at[k],
            device_id=where, device_id_type=MESH,
        )

    def fy1(k):
        return remote(fy1_s, fy1_r, fy1_ss, fy1_rs, k, {"fy": fy - 1})

    def bulk1(k):
        return remote(bulk1_s, bulk1_r, bulk1_ss, bulk1_rs, k, {"fx": fx - 1})

    def corner1(k):
        return remote(corner1_s, corner1_r, corner1_ss, corner1_rs, k, {"fx": fx - 1})

    def bulk2(k):
        return remote(bulk2_s, bulk2_r, bulk2_ss, bulk2_rs, k, {"fx": fx + 1})

    def corner2(k):
        return remote(corner2_s, corner2_r, corner2_ss, corner2_rs, k, {"fx": fx + 1})

    def to_relay(src, via, send, recv, k, offset):
        return remote(src, via, send, recv, k, {"fx": fx + offset})

    def via_bulk1(k):
        return to_relay(bulk1_s, via_bulk, bulk1_ss, via_bulk_rs, k, -RUN)

    def via_corner1(k):
        return to_relay(corner1_s, via_corner, corner1_ss, via_corner_rs, k, -RUN)

    def via_bulk2(k):
        return to_relay(bulk2_s, via_bulk, bulk2_ss, via_bulk_rs, k, RUN)

    def via_corner2(k):
        return to_relay(corner2_s, via_corner, corner2_ss, via_corner_rs, k, RUN)

    def on_bulk1(k):
        return to_relay(via_bulk, bulk1_r, via_bulk_ss, bulk1_rs, k, RUN - 1)

    def on_corner1(k):
        return to_relay(via_corner, corner1_r, via_corner_ss, corner1_rs, k, RUN - 1)

    def on_bulk2(k):
        return to_relay(via_bulk, bulk2_r, via_bulk_ss, bulk2_rs, k, 1 - RUN)

    def on_corner2(k):
        return to_relay(via_corner, corner2_r, via_corner_ss, corner2_rs, k, 1 - RUN)

    def leftward(direct, relay, k, action):
        pl.when(has_left)(lambda: by_relay(crosses_left, left_relayed(k), lambda: direct(k), lambda: relay(k), action))

    def rightward(direct, relay, k, action):
        pl.when(has_right)(lambda: by_relay(crosses_right, right_relayed(k), lambda: direct(k), lambda: relay(k), action))

    def start(copy):
        copy.start()

    def wait_send(copy):
        copy.wait_send()

    def carries1(k):
        return via1_here & among(RELAYED_LEFT, run, k)

    def carries2(k):
        return via2_here & among(RELAYED_RIGHT, run - 1, k)

    def relay1(k):
        @pl.when(carries1(k))
        def _():
            via_bulk1(k).wait_recv()
            on_bulk1(k).start()
            via_corner1(k).wait_recv()
            on_corner1(k).start()

    def relay2(k):
        @pl.when(carries2(k))
        def _():
            via_corner2(k).wait_recv()
            on_corner2(k).start()
            via_bulk2(k).wait_recv()
            on_bulk2(k).start()

    def fy2(k):
        return remote(fy2_s, fy2_r, fy2_ss, fy2_rs, k, {"fy": fy + 1})

    lane_e = lax.broadcasted_iota(jnp.int32, (ex, LANES), 1)
    lane_b = lax.broadcasted_iota(jnp.int32, (border, LANES), 1)
    lane_h = lax.broadcasted_iota(jnp.int32, (half, LANES), 1)
    low_edge = (lane_e >= tail - border) & (lane_e < tail)

    def roll(value, shift):
        shift = shift % LANES
        return pltpu.roll(value, shift, 1) if shift else value

    def pack_bulk(tile0, tile1, out, k):
        joined = jnp.zeros((border, LANES), jnp.float32)
        for c in range(GROUP):
            out[k, c * border : (c + 1) * border, :] = tile0(c)
            moved = roll(tile1(c), 32 * c)
            joined = jnp.where((lane_b >= 32 * c) & (lane_b < 32 * c + 32), moved, joined)
        out[k, GROUP * border : (GROUP + 1) * border, :] = joined

    def pack_corner(tile1, out, k):
        joined = jnp.zeros((border, LANES), jnp.float32)
        rest = jnp.zeros((half, LANES), jnp.float32)
        for c in range(GROUP):
            value = tile1(c)
            moved = roll(value, 32 * c - 32)
            joined = jnp.where((lane_b >= 32 * c) & (lane_b < 32 * c + 32), moved, joined)
            for part in range(2):
                to = part * 64 + c * 16
                moved = roll(value[part * half : (part + 1) * half], to - 64)
                rest = jnp.where((lane_h >= to) & (lane_h < to + 16), moved, rest)
        out[k, :border, :] = joined
        out[k, border:, :] = rest

    def unpack_corner(ref, k, c):
        middle = roll(ref[k, :border, :], 32 - 32 * c)
        parts = [roll(ref[k, border:, :], 64 - part * 64 - c * 16) for part in range(2)]
        return jnp.where(lane_b < 64, middle, jnp.concatenate(parts, axis=0))

    def unpack(bulk, corner, k, c):
        first = bulk[k, c * border : (c + 1) * border, :]
        start = roll(bulk[k, GROUP * border : (GROUP + 1) * border, :], -32 * c)
        return first, jnp.where(lane_b < 32, start, unpack_corner(corner, k, c))

    def put_rows(at, lanes, value):
        high = value.astype(jnp.bfloat16)
        rows_hi[at : at + ex, lanes] = high
        rows_lo[at : at + ex, lanes] = (value - high.astype(jnp.float32)).astype(jnp.bfloat16)

    def synthesize(k):
        load(dual_hbm, dual, dual_sem, k).wait()
        first = k * GROUP
        left = jnp.concatenate([dual[first + c, :, :LANES] for c in range(GROUP)], axis=1)
        from_left = dot3((lowx[0], lowx[1]), split(left))
        for c in range(GROUP):
            lanes = slice(c * LANES, (c + 1) * LANES)
            put_rows(c * ex, slice(0, LANES), from_left[:ex, lanes])
            put_rows(c * ex, slice(LANES, 2 * LANES), from_left[ex:, lanes])
        right = jnp.concatenate([dual[first + c, :, LANES:] for c in range(GROUP)], axis=1)
        from_right = dot3((wxt[0], wxt[1]), split(right))
        for c in range(GROUP):
            put_rows(c * ex, slice(2 * LANES, 3 * LANES), from_right[:, c * LANES : (c + 1) * LANES])
        result = dot3((rows_hi[...], rows_lo[...]), (ay[0], ay[1]))
        for c in range(GROUP):
            work[first + c] = result[c * ex : (c + 1) * ex]

        @pl.when(k == 0)
        def _():
            pl.semaphore_wait(barrier, neighbours)

        for p in range(GROUP // 2):
            a, b = work[first + 2 * p, :, LANES:], work[first + 2 * p + 1, :, LANES:]
            fy1_s[k, p] = jnp.where(low_edge, roll(a, -border), roll(b, 64 - border))
        pl.when(has_up)(lambda: fy1(k).start())

    def send_bulk(k):
        first = k * GROUP
        pack_bulk(
            lambda c: work[first + c, :border, :LANES], lambda c: work[first + c, :border, LANES:], bulk1_s, k
        )
        leftward(bulk1, via_bulk1, k, start)

    def send_columns(k):
        pl.when(has_down)(lambda: fy1(k).wait_recv())
        for p in range(GROUP // 2):
            a = k * GROUP + 2 * p
            strip = fy1_r[k, p]
            work[a, :, LANES:] = work[a, :, LANES:] + jnp.where(low_edge, strip, 0.0)
            work[a + 1, :, LANES:] = work[a + 1, :, LANES:] + jnp.where(low_edge, roll(strip, 64), 0.0)
        pack_corner(lambda c: work[k * GROUP + c, :border, LANES:], corner1_s, k)
        leftward(corner1, via_corner1, k, start)

    root = jnp.float32(0.5**0.5)

    def weights(lane_from):
        rows = lax.broadcasted_iota(jnp.int32, (tx, LANES), 0)
        lanes = lax.broadcasted_iota(jnp.int32, (tx, LANES), 1) + lane_from
        by_x = jnp.where((rows >= tx - border) & has_right, root, 1.0)
        by_y = jnp.where((lanes >= ty - border) & has_down, root, 1.0)
        return by_x * by_y

    def update_image(k):
        load(img_hbm, img, img_sem, k).wait()
        load(grad_hbm, grad, grad_sem, k).wait()

        @pl.when(has_right)
        def _():
            bulk1(k).wait_recv()
            corner1(k).wait_recv()

        keep = tx - border
        w0 = weights(0)
        w1 = weights(LANES)[:, :tail]
        for c in range(GROUP):
            i = k * GROUP + c
            add0, add1 = unpack(bulk1_r, corner1_r, k, c)
            for own, add, w, lanes in (
                (work[i, border:, :LANES], add0, w0, slice(0, LANES)),
                (work[i, border:, LANES:ty], add1[:, :tail], w1, slice(LANES, ty)),
            ):
                summed = jnp.concatenate([own[:keep], own[keep:] + add], axis=0)
                image = img[i, :, lanes]
                step = jnp.maximum(image - TAU_STEP * (grad[i, :, lanes].astype(jnp.float32) + summed * w), 0.0)
                image_next[i, :, lanes] = step
                work[i, border:, lanes] = (2.0 * step - image) * w
        pack_corner(lambda c: work[k * GROUP + c, tx:, LANES:], corner2_s, k)
        rightward(corner2, via_corner2, k, start)
        pack_bulk(
            lambda c: work[k * GROUP + c, tx:, :LANES], lambda c: work[k * GROUP + c, tx:, LANES:], bulk2_s, k
        )
        rightward(bulk2, via_bulk2, k, start)

    def send_rows(k):
        pl.when(has_left)(lambda: corner2(k).wait_recv())
        for p in range(GROUP // 2):
            a, b = [
                jnp.concatenate([unpack_corner(corner2_r, k, c), work[k * GROUP + c, border:, LANES:]], axis=0)
                for c in (2 * p, 2 * p + 1)
            ]
            fy2_s[k, p] = jnp.where(lane_e >= tail, roll(a, border), roll(b, 64 + border))
        pl.when(has_down)(lambda: fy2(k).start())

    def analyse(k):
        @pl.when(k == 0)
        def _():
            for i in range(3, len(constants)):
                constant(i).wait()

        pl.when(has_left)(lambda: bulk2(k).wait_recv())
        pl.when(has_up)(lambda: fy2(k).wait_recv())
        first = k * GROUP
        for c in range(GROUP):
            i = first + c
            strip = roll(fy2_r[k, c // 2], 64 * (c % 2))
            edge0, edge1 = unpack(bulk2_r, corner2_r, k, c)
            put_rows(c * ex, slice(0, LANES), jnp.concatenate([edge0, work[i, border:, :LANES]], axis=0))
            second = jnp.concatenate([edge1, work[i, border:, LANES:]], axis=0)
            put_rows(c * ex, slice(LANES, 2 * LANES), jnp.where(lane_e < tail, second, strip))
        mixed[...] = dot3((rows_hi[:, :ey], rows_lo[:, :ey]), (ayt[0], ayt[1]))

        def beside(tile):
            lanes = slice(tile * LANES, (tile + 1) * LANES)
            return jnp.concatenate([mixed[c * ex : (c + 1) * ex, lanes] for c in range(GROUP)], axis=1)

        low = dot3((lowxt[0], lowxt[1]), split(jnp.concatenate([beside(0), beside(1)], axis=0)))
        high = dot3((wx[0], wx[1]), split(beside(2)))
        for lanes, part in ((slice(0, LANES), low), (slice(LANES, 2 * LANES), high)):
            squares = total[:, lanes]
            for c in range(GROUP):
                value = dual[first + c, :, lanes] + part[:, c * LANES : (c + 1) * LANES]
                updated[first + c, :, lanes] = value
                squares = squares + value * value
            total[:, lanes] = squares

    for i in range(3):
        constant(i).wait()
    for k in range(1, chunks):
        load(dual_hbm, dual, dual_sem, k).start()
    for k in range(chunks):
        load(img_hbm, img, img_sem, k).start()
        load(grad_hbm, grad, grad_sem, k).start()
    for i in range(3, len(constants)):
        constant(i).start()

    image_lag, rows_lag = [jnp.where(crosses_right, *lags) for lags in (IMAGE_LAG, ROWS_LAG)]
    phases = (
        (synthesize, 0), (send_columns, 2), (send_bulk, 0), (relay1, RELAY_LAG[0]), (update_image, image_lag),
        (relay2, RELAY_LAG[1]), (send_rows, rows_lag), (analyse, rows_lag + 1),
    )
    if not relays:
        phases = tuple(p for p in phases if p[0] not in (relay1, relay2))

    def step(s, carry):
        for phase, lag in phases:

            @pl.when((s >= lag) & (s < chunks + lag))
            def _(phase=phase, lag=lag):
                phase(s - lag)

        return carry

    lax.fori_loop(0, chunks + rows_lag + 1, step, 0)

    swap = pltpu.make_async_remote_copy(
        src_ref=total, dst_ref=other, send_sem=ch_ss, recv_sem=ch_rs, device_id={"ch": 1 - ch}, device_id_type=MESH
    )
    swap.start()

    def drain(k, carry):
        pl.when(has_up)(lambda: fy1(k).wait_send())

        leftward(bulk1, via_bulk1, k, wait_send)
        leftward(corner1, via_corner1, k, wait_send)
        rightward(corner2, via_corner2, k, wait_send)
        rightward(bulk2, via_bulk2, k, wait_send)
        if relays:

            @pl.when(carries1(k))
            def _():
                on_bulk1(k).wait_send()
                on_corner1(k).wait_send()

            @pl.when(carries2(k))
            def _():
                on_bulk2(k).wait_send()
                on_corner2(k).wait_send()

        pl.when(has_down)(lambda: fy2(k).wait_send())
        return carry

    lax.fori_loop(0, chunks, drain, 0)
    swap.wait()
    factor[...] = jnp.minimum(1.0, LAMBDA_REG * rw[...] / jnp.sqrt(total[...] + other[...] + EPSILON))


def finish(chunks, image, updated, factor, image_out, dual_out, scaled, image_sem, sems):
    pltpu.make_async_copy(image, image_out, image_sem).start()

    def copy(k):
        rows = pl.ds(k * GROUP, GROUP)
        return pltpu.make_async_copy(scaled.at[rows], dual_out.at[rows], sems.at[k])

    def step(k, carry):
        for c in range(GROUP):
            scaled[k * GROUP + c] = updated[k * GROUP + c] * factor[...]
        copy(k).start()
        return carry

    lax.fori_loop(0, chunks, step, 0)
    pltpu.make_async_copy(image, image_out, image_sem).wait()

    def drain(k, carry):
        copy(k).wait()
        return carry

    lax.fori_loop(0, chunks, drain, 0)


def shards(mesh_shape, image_cube, data_grad, dual_coeffs, reweights):
    channels, tx, ty = image_cube.shape
    _, ex, ey = dual_coeffs.shape
    border = ex - tx
    chunks = channels // GROUP
    constants = [jnp.asarray(m) for m in matrices(ex, ey, border)]
    sizes = (mesh_shape["fx"], mesh_shape["fy"], chunks, tx, ty, border)
    f32, bf16 = jnp.float32, jnp.bfloat16
    strip_y = pltpu.VMEM((chunks, GROUP // 2, ex, LANES), f32)
    bulk = pltpu.VMEM((chunks, (GROUP + 1) * border, LANES), f32)
    corner = pltpu.VMEM((chunks, border + border // 2, LANES), f32)
    dma = pltpu.SemaphoreType.DMA
    in_hbm = pl.BlockSpec(memory_space=pltpu.HBM)
    in_vmem = pl.BlockSpec(memory_space=pltpu.VMEM)
    operands = [
        pltpu.with_memory_space_constraint(x, pltpu.HBM)
        for x in (image_cube, data_grad, dual_coeffs, reweights, *constants)
    ]
    image_next, updated, factor = pl.pallas_call(
        functools.partial(kernel, sizes),
        out_shape=(
            jax.ShapeDtypeStruct(image_cube.shape, f32),
            jax.ShapeDtypeStruct(dual_coeffs.shape, f32),
            jax.ShapeDtypeStruct(reweights.shape, f32),
        ),
        in_specs=[in_hbm] * len(operands),
        out_specs=(in_vmem,) * 3,
        scratch_shapes=[
            pltpu.VMEM(image_cube.shape, f32),
            pltpu.VMEM(data_grad.shape, data_grad.dtype),
            pltpu.VMEM(dual_coeffs.shape, f32),
            pltpu.VMEM(reweights.shape, f32),
            *[pltpu.VMEM(m.shape, m.dtype) for m in constants],
            pltpu.VMEM(dual_coeffs.shape, f32),
            pltpu.VMEM((GROUP * ex, ey + LANES), bf16),
            pltpu.VMEM((GROUP * ex, ey + LANES), bf16),
            pltpu.VMEM((GROUP * ex, ey + LANES), f32),
            strip_y, strip_y, bulk, bulk, corner, corner, bulk, bulk, corner, corner, strip_y, strip_y, bulk, corner,
            pltpu.VMEM((ex, ey), f32), pltpu.VMEM((ex, ey), f32),
            dma((chunks,)), dma((chunks,)), dma((chunks,)), dma((7,)),
            *[dma((chunks,)) for _ in range(16)],
            dma, dma,
        ],
        compiler_params=pltpu.CompilerParams(
            collective_id=0, has_side_effects=True, vmem_limit_bytes=40 * 2**20
        ),
        name="primal_dual",
    )(*operands)
    return pl.pallas_call(
        functools.partial(finish, chunks),
        out_shape=(
            jax.ShapeDtypeStruct(image_cube.shape, f32),
            jax.ShapeDtypeStruct(dual_coeffs.shape, f32),
        ),
        in_specs=[in_vmem] * 3,
        out_specs=(in_hbm,) * 2,
        scratch_shapes=[pltpu.VMEM(dual_coeffs.shape, f32), dma, dma((chunks,))],
        compiler_params=pltpu.CompilerParams(vmem_limit_bytes=16 * 2**20),
        name="scaled_results",
    )(image_next, updated, factor)


def solution(mesh):
    return jax.shard_map(
        functools.partial(shards, dict(mesh.shape)),
        mesh=mesh,
        in_specs=(P("ch", "fx", "fy"), P("ch", "fx", "fy"), P("ch", "fx", "fy"), P("fx", "fy")),
        out_specs=(P("ch", "fx", "fy"), P("ch", "fx", "fy")),
        check_vma=False,
    )
```

```python
import functools

import jax
import jax.numpy as jnp
import numpy as np
from jax import lax
from jax.experimental import pallas as pl
from jax.experimental.pallas import tpu as pltpu
from jax.sharding import PartitionSpec as P

LOW_PASS = [
    -0.00011747678400228192,
    0.0006754494059985568,
    -0.0003917403729959771,
    -0.00487035299301066,
    0.008746094047015655,
    0.013981027917015516,
    -0.04408825393106472,
    -0.01736930100202211,
    0.128747426620186,
    0.00047248457399797254,
    -0.2840155429624281,
    -0.015829105256023893,
    0.5853546836548691,
    0.6756307362980128,
    0.3128715909144659,
    0.05441584224308161,
]
TAU_STEP = 0.5
LAMBDA_REG = 1.0
EPSILON = 1e-06
LANES = 128
GROUP = 4
RUN = 4
RELAYED_LEFT = ((0, 1, 3, 4, 6), (1, 3, 5), (3,))
RELAYED_RIGHT = ((2, 6), (0, 2, 4, 6), (0, 1, 2, 4, 5, 6))
IMAGE_LAG = (5, 8)
ROWS_LAG = (13, 16)
RELAY_LAG = (3, 7)
MESH = pl.DeviceIdType.MESH


def level_matrix(length):
    halved = length // 2
    taps_count = len(LOW_PASS)
    matrix = np.zeros((length, length))
    for out_row in range(halved):
        for tap_index in range(taps_count):
            column = (2 * out_row + tap_index) % length
            matrix[out_row, column] += LOW_PASS[tap_index]
            matrix[halved + out_row, column] += (-1) ** tap_index * LOW_PASS[
                taps_count - 1 - tap_index
            ]
    return matrix


def split_np(matrix):
    single = matrix.astype(np.float32)
    high = single.astype(jnp.bfloat16)
    low = (single - high.astype(np.float32)).astype(jnp.bfloat16)
    return np.stack([high, low])


def matrices(ex, ey, border):
    wx, wy = level_matrix(ex), level_matrix(ey)
    hx, hy = ex // 2, ey // 2
    along_y = np.concatenate([level_matrix(hy) @ wy[:hy], wy], axis=0)
    order = np.concatenate([np.arange(border, ey), np.arange(border)])
    along_y = along_y[:, order]
    low_x = np.zeros((2 * ex, ex))
    low_x[:ex, :hx] = (level_matrix(hx) @ wx[:hx]).T
    low_x[ex:, hx:] = wx[hx:].T
    return [
        split_np(low_x),
        split_np(wx.T),
        split_np(along_y),
        split_np(along_y.T),
        split_np(low_x.T),
        split_np(wx),
    ]


def split(value):
    high = value.astype(jnp.bfloat16)
    low = (value - high.astype(jnp.float32)).astype(jnp.bfloat16)
    return high, low


def dot3(a, b):
    dot = functools.partial(jnp.dot, preferred_element_type=jnp.float32)
    return dot(a[0], b[0]) + (dot(a[0], b[1]) + dot(a[1], b[0]))


def kernel(
    sizes,
    img_hbm, grad_hbm, dual_hbm, rw_hbm, lowx_hbm, wxt_hbm, ay_hbm, ayt_hbm, lowxt_hbm, wx_hbm,
    image_next, updated, factor,
    img, grad, dual, rw, lowx, wxt, ay, ayt, lowxt, wx,
    work, rows_hi, rows_lo, mixed,
    fy1_s, fy1_r, bulk1_s, bulk1_r, corner1_s, corner1_r,
    bulk2_s, bulk2_r, corner2_s, corner2_r, fy2_s, fy2_r, via_bulk, via_corner, total, other,
    dual_sem, img_sem, grad_sem, const_sem,
    fy1_ss, fy1_rs, bulk1_ss, bulk1_rs, corner1_ss, corner1_rs,
    bulk2_ss, bulk2_rs, corner2_ss, corner2_rs, fy2_ss, fy2_rs,
    via_bulk_ss, via_bulk_rs, via_corner_ss, via_corner_rs, ch_ss, ch_rs,
):
    n_fx, n_fy, chunks, tx, ty, border = sizes
    ex = tx + border
    ey = ty + border
    tail = ty - LANES
    half = border // 2
    fx, fy, ch = lax.axis_index("fx"), lax.axis_index("fy"), lax.axis_index("ch")
    has_left, has_right = fx > 0, fx < n_fx - 1
    has_up, has_down = fy > 0, fy < n_fy - 1

    relays = n_fx == RUN * RUN
    run, place = fx // RUN, fx % RUN
    at_first, at_last = place == 0, place == RUN - 1
    if relays:
        crosses_left, crosses_right = at_first & has_left, at_last & has_right
        via1_here, via2_here = at_first & (run < RUN - 1), at_last & (run > 0)
    else:
        crosses_left = crosses_right = via1_here = via2_here = False

    def among(chosen, pair, k):
        found = False
        for index, listed in enumerate(chosen):
            for member in listed:
                found = found | ((pair == index) & (k == member))
        return found

    def by_relay(crosses, relayed, direct, relay, action):
        if not relays:
            return action(direct())
        pl.when(crosses & relayed)(lambda: action(relay()))
        pl.when(jnp.logical_not(crosses & relayed))(lambda: action(direct()))

    def left_relayed(k):
        return among(RELAYED_LEFT, run - 1, k)

    def right_relayed(k):
        return among(RELAYED_RIGHT, run, k)

    barrier = pltpu.get_barrier_semaphore()

    def greet(condition, where):
        @pl.when(condition)
        def _():
            pl.semaphore_signal(barrier, inc=1, device_id=where, device_id_type=MESH)

    greet(has_left, {"fx": fx - 1})
    greet(has_right, {"fx": fx + 1})
    greet(has_up, {"fy": fy - 1})
    greet(has_down, {"fy": fy + 1})
    pl.semaphore_signal(barrier, inc=1, device_id={"ch": 1 - ch}, device_id_type=MESH)
    neighbours = 1 + sum(c.astype(jnp.int32) for c in (has_left, has_right, has_up, has_down))
    if relays:
        ends = at_first | at_last
        for condition, offset in (
            (ends & (run > 0), -RUN), (ends & (run < RUN - 1), RUN), (at_first, RUN - 1), (at_last, 1 - RUN)
        ):
            greet(condition, {"fx": fx + offset})
            neighbours = neighbours + condition.astype(jnp.int32)

    def load(src, dst, sems, k):
        rows = pl.ds(k * GROUP, GROUP)
        return pltpu.make_async_copy(src.at[rows], dst.at[rows], sems.at[k])

    constants = [
        (lowx_hbm, lowx), (wxt_hbm, wxt), (ay_hbm, ay), (ayt_hbm, ayt), (lowxt_hbm, lowxt), (wx_hbm, wx), (rw_hbm, rw)
    ]

    def constant(i):
        return pltpu.make_async_copy(constants[i][0], constants[i][1], const_sem.at[i])

    load(dual_hbm, dual, dual_sem, 0).start()
    for i in range(3):
        constant(i).start()
    def clear(condition, *refs):
        @pl.when(condition)
        def _():
            for ref in refs:
                ref[...] = jnp.zeros_like(ref)

    clear(fy == n_fy - 1, fy1_r)
    clear(fx == n_fx - 1, bulk1_r, corner1_r)
    clear(fx == 0, bulk2_r, corner2_r)
    clear(fy == 0, fy2_r)
    total[...] = jnp.zeros_like(total)

    def remote(src, dst, send, recv, k, where):
        return pltpu.make_async_remote_copy(
            src_ref=src.at[k], dst_ref=dst.at[k], send_sem=send.at[k], recv_sem=recv.at[k],
            device_id=where, device_id_type=MESH,
        )

    def fy1(k):
        return remote(fy1_s, fy1_r, fy1_ss, fy1_rs, k, {"fy": fy - 1})

    def bulk1(k):
        return remote(bulk1_s, bulk1_r, bulk1_ss, bulk1_rs, k, {"fx": fx - 1})

    def corner1(k):
        return remote(corner1_s, corner1_r, corner1_ss, corner1_rs, k, {"fx": fx - 1})

    def bulk2(k):
        return remote(bulk2_s, bulk2_r, bulk2_ss, bulk2_rs, k, {"fx": fx + 1})

    def corner2(k):
        return remote(corner2_s, corner2_r, corner2_ss, corner2_rs, k, {"fx": fx + 1})

    def to_relay(src, via, send, recv, k, offset):
        return remote(src, via, send, recv, k, {"fx": fx + offset})

    def via_bulk1(k):
        return to_relay(bulk1_s, via_bulk, bulk1_ss, via_bulk_rs, k, -RUN)

    def via_corner1(k):
        return to_relay(corner1_s, via_corner, corner1_ss, via_corner_rs, k, -RUN)

    def via_bulk2(k):
        return to_relay(bulk2_s, via_bulk, bulk2_ss, via_bulk_rs, k, RUN)

    def via_corner2(k):
        return to_relay(corner2_s, via_corner, corner2_ss, via_corner_rs, k, RUN)

    def on_bulk1(k):
        return to_relay(via_bulk, bulk1_r, via_bulk_ss, bulk1_rs, k, RUN - 1)

    def on_corner1(k):
        return to_relay(via_corner, corner1_r, via_corner_ss, corner1_rs, k, RUN - 1)

    def on_bulk2(k):
        return to_relay(via_bulk, bulk2_r, via_bulk_ss, bulk2_rs, k, 1 - RUN)

    def on_corner2(k):
        return to_relay(via_corner, corner2_r, via_corner_ss, corner2_rs, k, 1 - RUN)

    def leftward(direct, relay, k, action):
        pl.when(has_left)(lambda: by_relay(crosses_left, left_relayed(k), lambda: direct(k), lambda: relay(k), action))

    def rightward(direct, relay, k, action):
        pl.when(has_right)(lambda: by_relay(crosses_right, right_relayed(k), lambda: direct(k), lambda: relay(k), action))

    def start(copy):
        copy.start()

    def wait_send(copy):
        copy.wait_send()

    def carries1(k):
        return via1_here & among(RELAYED_LEFT, run, k)

    def carries2(k):
        return via2_here & among(RELAYED_RIGHT, run - 1, k)

    def relay1(k):
        @pl.when(carries1(k))
        def _():
            via_bulk1(k).wait_recv()
            on_bulk1(k).start()
            via_corner1(k).wait_recv()
            on_corner1(k).start()

    def relay2(k):
        @pl.when(carries2(k))
        def _():
            via_corner2(k).wait_recv()
            on_corner2(k).start()
            via_bulk2(k).wait_recv()
            on_bulk2(k).start()

    def fy2(k):
        return remote(fy2_s, fy2_r, fy2_ss, fy2_rs, k, {"fy": fy + 1})

    def swap(side):
        return remote(total, other, ch_ss, ch_rs, side, {"ch": 1 - ch})

    lane_e = lax.broadcasted_iota(jnp.int32, (ex, LANES), 1)
    lane_b = lax.broadcasted_iota(jnp.int32, (border, LANES), 1)
    lane_h = lax.broadcasted_iota(jnp.int32, (half, LANES), 1)
    low_edge = (lane_e >= tail - border) & (lane_e < tail)

    def roll(value, shift):
        shift = shift % LANES
        return pltpu.roll(value, shift, 1) if shift else value

    def pack_bulk(tile0, tile1, out, k):
        joined = jnp.zeros((border, LANES), jnp.float32)
        for c in range(GROUP):
            out[k, c * border : (c + 1) * border, :] = tile0(c)
            moved = roll(tile1(c), 32 * c)
            joined = jnp.where((lane_b >= 32 * c) & (lane_b < 32 * c + 32), moved, joined)
        out[k, GROUP * border : (GROUP + 1) * border, :] = joined

    def pack_corner(tile1, out, k):
        joined = jnp.zeros((border, LANES), jnp.float32)
        rest = jnp.zeros((half, LANES), jnp.float32)
        for c in range(GROUP):
            value = tile1(c)
            moved = roll(value, 32 * c - 32)
            joined = jnp.where((lane_b >= 32 * c) & (lane_b < 32 * c + 32), moved, joined)
            for part in range(2):
                to = part * 64 + c * 16
                moved = roll(value[part * half : (part + 1) * half], to - 64)
                rest = jnp.where((lane_h >= to) & (lane_h < to + 16), moved, rest)
        out[k, :border, :] = joined
        out[k, border:, :] = rest

    def unpack_corner(ref, k, c):
        middle = roll(ref[k, :border, :], 32 - 32 * c)
        parts = [roll(ref[k, border:, :], 64 - part * 64 - c * 16) for part in range(2)]
        return jnp.where(lane_b < 64, middle, jnp.concatenate(parts, axis=0))

    def unpack(bulk, corner, k, c):
        first = bulk[k, c * border : (c + 1) * border, :]
        start = roll(bulk[k, GROUP * border : (GROUP + 1) * border, :], -32 * c)
        return first, jnp.where(lane_b < 32, start, unpack_corner(corner, k, c))

    def put_rows(at, lanes, value):
        high = value.astype(jnp.bfloat16)
        rows_hi[at : at + ex, lanes] = high
        rows_lo[at : at + ex, lanes] = (value - high.astype(jnp.float32)).astype(jnp.bfloat16)

    def synthesize(k):
        load(dual_hbm, dual, dual_sem, k).wait()
        first = k * GROUP
        left = jnp.concatenate([dual[first + c, :, :LANES] for c in range(GROUP)], axis=1)
        from_left = dot3((lowx[0], lowx[1]), split(left))
        for c in range(GROUP):
            lanes = slice(c * LANES, (c + 1) * LANES)
            put_rows(c * ex, slice(0, LANES), from_left[:ex, lanes])
            put_rows(c * ex, slice(LANES, 2 * LANES), from_left[ex:, lanes])
        right = jnp.concatenate([dual[first + c, :, LANES:] for c in range(GROUP)], axis=1)
        from_right = dot3((wxt[0], wxt[1]), split(right))
        for c in range(GROUP):
            put_rows(c * ex, slice(2 * LANES, 3 * LANES), from_right[:, c * LANES : (c + 1) * LANES])
        result = dot3((rows_hi[...], rows_lo[...]), (ay[0], ay[1]))
        for c in range(GROUP):
            work[first + c] = result[c * ex : (c + 1) * ex]

        @pl.when(k == 0)
        def _():
            pl.semaphore_wait(barrier, neighbours)

        for p in range(GROUP // 2):
            a, b = work[first + 2 * p, :, LANES:], work[first + 2 * p + 1, :, LANES:]
            fy1_s[k, p] = jnp.where(low_edge, roll(a, -border), roll(b, 64 - border))
        pl.when(has_up)(lambda: fy1(k).start())

    def send_bulk(k):
        first = k * GROUP
        pack_bulk(
            lambda c: work[first + c, :border, :LANES], lambda c: work[first + c, :border, LANES:], bulk1_s, k
        )
        leftward(bulk1, via_bulk1, k, start)

    def send_columns(k):
        pl.when(has_down)(lambda: fy1(k).wait_recv())
        for p in range(GROUP // 2):
            a = k * GROUP + 2 * p
            strip = fy1_r[k, p]
            work[a, :, LANES:] = work[a, :, LANES:] + jnp.where(low_edge, strip, 0.0)
            work[a + 1, :, LANES:] = work[a + 1, :, LANES:] + jnp.where(low_edge, roll(strip, 64), 0.0)
        pack_corner(lambda c: work[k * GROUP + c, :border, LANES:], corner1_s, k)
        leftward(corner1, via_corner1, k, start)

    root = jnp.float32(0.5**0.5)

    def weights(lane_from):
        rows = lax.broadcasted_iota(jnp.int32, (tx, LANES), 0)
        lanes = lax.broadcasted_iota(jnp.int32, (tx, LANES), 1) + lane_from
        by_x = jnp.where((rows >= tx - border) & has_right, root, 1.0)
        by_y = jnp.where((lanes >= ty - border) & has_down, root, 1.0)
        return by_x * by_y

    def update_image(k):
        load(img_hbm, img, img_sem, k).wait()
        load(grad_hbm, grad, grad_sem, k).wait()

        @pl.when(has_right)
        def _():
            bulk1(k).wait_recv()
            corner1(k).wait_recv()

        keep = tx - border
        w0 = weights(0)
        w1 = weights(LANES)[:, :tail]
        for c in range(GROUP):
            i = k * GROUP + c
            add0, add1 = unpack(bulk1_r, corner1_r, k, c)
            for own, add, w, lanes in (
                (work[i, border:, :LANES], add0, w0, slice(0, LANES)),
                (work[i, border:, LANES:ty], add1[:, :tail], w1, slice(LANES, ty)),
            ):
                summed = jnp.concatenate([own[:keep], own[keep:] + add], axis=0)
                image = img[i, :, lanes]
                step = jnp.maximum(image - TAU_STEP * (grad[i, :, lanes].astype(jnp.float32) + summed * w), 0.0)
                image_next[i, :, lanes] = step
                work[i, border:, lanes] = (2.0 * step - image) * w
        pack_corner(lambda c: work[k * GROUP + c, tx:, LANES:], corner2_s, k)
        rightward(corner2, via_corner2, k, start)
        pack_bulk(
            lambda c: work[k * GROUP + c, tx:, :LANES], lambda c: work[k * GROUP + c, tx:, LANES:], bulk2_s, k
        )
        rightward(bulk2, via_bulk2, k, start)

    def send_rows(k):
        pl.when(has_left)(lambda: corner2(k).wait_recv())
        for p in range(GROUP // 2):
            a, b = [
                jnp.concatenate([unpack_corner(corner2_r, k, c), work[k * GROUP + c, border:, LANES:]], axis=0)
                for c in (2 * p, 2 * p + 1)
            ]
            fy2_s[k, p] = jnp.where(lane_e >= tail, roll(a, border), roll(b, 64 + border))
        pl.when(has_down)(lambda: fy2(k).start())

    def analyse(k):
        @pl.when(k == 0)
        def _():
            for i in range(3, len(constants)):
                constant(i).wait()

        pl.when(has_left)(lambda: bulk2(k).wait_recv())
        pl.when(has_up)(lambda: fy2(k).wait_recv())
        first = k * GROUP
        for c in range(GROUP):
            i = first + c
            strip = roll(fy2_r[k, c // 2], 64 * (c % 2))
            edge0, edge1 = unpack(bulk2_r, corner2_r, k, c)
            put_rows(c * ex, slice(0, LANES), jnp.concatenate([edge0, work[i, border:, :LANES]], axis=0))
            second = jnp.concatenate([edge1, work[i, border:, LANES:]], axis=0)
            put_rows(c * ex, slice(LANES, 2 * LANES), jnp.where(lane_e < tail, second, strip))
        mixed[...] = dot3((rows_hi[:, :ey], rows_lo[:, :ey]), (ayt[0], ayt[1]))

        def beside(tile):
            lanes = slice(tile * LANES, (tile + 1) * LANES)
            return jnp.concatenate([mixed[c * ex : (c + 1) * ex, lanes] for c in range(GROUP)], axis=1)

        for side, matrix, tiles in ((0, lowxt, (0, 1)), (1, wx, (2,))):
            lanes = slice(side * LANES, (side + 1) * LANES)
            part = dot3((matrix[0], matrix[1]), split(jnp.concatenate([beside(t) for t in tiles], axis=0)))
            squares = total[side]
            for c in range(GROUP):
                value = dual[first + c, :, lanes] + part[:, c * LANES : (c + 1) * LANES]
                updated[first + c, :, lanes] = value
                squares = squares + value * value
            total[side] = squares
            pl.when(k == chunks - 1)(lambda side=side: swap(side).start())

    for i in range(3):
        constant(i).wait()
    for k in range(1, chunks):
        load(dual_hbm, dual, dual_sem, k).start()
    for k in range(chunks):
        load(img_hbm, img, img_sem, k).start()
        load(grad_hbm, grad, grad_sem, k).start()
    for i in range(3, len(constants)):
        constant(i).start()

    image_lag, rows_lag = [jnp.where(crosses_right, *lags) for lags in (IMAGE_LAG, ROWS_LAG)]
    phases = (
        (synthesize, 0), (send_columns, 2), (send_bulk, 0), (relay1, RELAY_LAG[0]), (update_image, image_lag),
        (relay2, RELAY_LAG[1]), (send_rows, rows_lag), (analyse, rows_lag + 1),
    )
    if not relays:
        phases = tuple(p for p in phases if p[0] not in (relay1, relay2))

    def step(s, carry):
        for phase, lag in phases:

            @pl.when((s >= lag) & (s < chunks + lag))
            def _(phase=phase, lag=lag):
                phase(s - lag)

        return carry

    lax.fori_loop(0, chunks + rows_lag + 1, step, 0)

    def drain(k, carry):
        pl.when(has_up)(lambda: fy1(k).wait_send())

        leftward(bulk1, via_bulk1, k, wait_send)
        leftward(corner1, via_corner1, k, wait_send)
        rightward(corner2, via_corner2, k, wait_send)
        rightward(bulk2, via_bulk2, k, wait_send)
        if relays:

            @pl.when(carries1(k))
            def _():
                on_bulk1(k).wait_send()
                on_corner1(k).wait_send()

            @pl.when(carries2(k))
            def _():
                on_bulk2(k).wait_send()
                on_corner2(k).wait_send()

        pl.when(has_down)(lambda: fy2(k).wait_send())
        return carry

    lax.fori_loop(0, chunks, drain, 0)
    for side in range(2):
        lanes = slice(side * LANES, (side + 1) * LANES)
        swap(side).wait()
        factor[:, lanes] = jnp.minimum(1.0, LAMBDA_REG * rw[:, lanes] * lax.rsqrt(total[side] + other[side] + EPSILON))


def finish(chunks, image, updated, factor, image_out, dual_out, scaled, image_sems, sems):
    def copies(k):
        rows = pl.ds(k * GROUP, GROUP)
        return (
            pltpu.make_async_copy(scaled.at[rows], dual_out.at[rows], sems.at[k]),
            pltpu.make_async_copy(image.at[rows], image_out.at[rows], image_sems.at[k]),
        )

    def step(k, carry):
        dual_copy, image_copy = copies(k)
        image_copy.start()
        for c in range(GROUP):
            scaled[k * GROUP + c] = updated[k * GROUP + c] * factor[...]
        dual_copy.start()
        return carry

    lax.fori_loop(0, chunks, step, 0)

    def drain(k, carry):
        for copy in copies(k):
            copy.wait()
        return carry

    lax.fori_loop(0, chunks, drain, 0)


def shards(mesh_shape, image_cube, data_grad, dual_coeffs, reweights):
    channels, tx, ty = image_cube.shape
    _, ex, ey = dual_coeffs.shape
    border = ex - tx
    chunks = channels // GROUP
    constants = [jnp.asarray(m) for m in matrices(ex, ey, border)]
    sizes = (mesh_shape["fx"], mesh_shape["fy"], chunks, tx, ty, border)
    f32, bf16 = jnp.float32, jnp.bfloat16
    strip_y = pltpu.VMEM((chunks, GROUP // 2, ex, LANES), f32)
    bulk = pltpu.VMEM((chunks, (GROUP + 1) * border, LANES), f32)
    corner = pltpu.VMEM((chunks, border + border // 2, LANES), f32)
    dma = pltpu.SemaphoreType.DMA
    in_hbm = pl.BlockSpec(memory_space=pltpu.HBM)
    in_vmem = pl.BlockSpec(memory_space=pltpu.VMEM)
    operands = [
        pltpu.with_memory_space_constraint(x, pltpu.HBM)
        for x in (image_cube, data_grad, dual_coeffs, reweights, *constants)
    ]
    image_next, updated, factor = pl.pallas_call(
        functools.partial(kernel, sizes),
        out_shape=(
            jax.ShapeDtypeStruct(image_cube.shape, f32),
            jax.ShapeDtypeStruct(dual_coeffs.shape, f32),
            jax.ShapeDtypeStruct(reweights.shape, f32),
        ),
        in_specs=[in_hbm] * len(operands),
        out_specs=(in_vmem,) * 3,
        scratch_shapes=[
            pltpu.VMEM(image_cube.shape, f32),
            pltpu.VMEM(data_grad.shape, data_grad.dtype),
            pltpu.VMEM(dual_coeffs.shape, f32),
            pltpu.VMEM(reweights.shape, f32),
            *[pltpu.VMEM(m.shape, m.dtype) for m in constants],
            pltpu.VMEM(dual_coeffs.shape, f32),
            pltpu.VMEM((GROUP * ex, ey + LANES), bf16),
            pltpu.VMEM((GROUP * ex, ey + LANES), bf16),
            pltpu.VMEM((GROUP * ex, ey + LANES), f32),
            strip_y, strip_y, bulk, bulk, corner, corner, bulk, bulk, corner, corner, strip_y, strip_y, bulk, corner,
            pltpu.VMEM((2, ex, LANES), f32), pltpu.VMEM((2, ex, LANES), f32),
            dma((chunks,)), dma((chunks,)), dma((chunks,)), dma((7,)),
            *[dma((chunks,)) for _ in range(16)],
            dma((2,)), dma((2,)),
        ],
        compiler_params=pltpu.CompilerParams(
            collective_id=0, has_side_effects=True, vmem_limit_bytes=40 * 2**20
        ),
        name="primal_dual",
    )(*operands)
    return pl.pallas_call(
        functools.partial(finish, chunks),
        out_shape=(
            jax.ShapeDtypeStruct(image_cube.shape, f32),
            jax.ShapeDtypeStruct(dual_coeffs.shape, f32),
        ),
        in_specs=[in_vmem] * 3,
        out_specs=(in_hbm,) * 2,
        scratch_shapes=[pltpu.VMEM(dual_coeffs.shape, f32), dma((chunks,)), dma((chunks,))],
        compiler_params=pltpu.CompilerParams(vmem_limit_bytes=16 * 2**20),
        name="scaled_results",
    )(image_next, updated, factor)


def solution(mesh):
    return jax.shard_map(
        functools.partial(shards, dict(mesh.shape)),
        mesh=mesh,
        in_specs=(P("ch", "fx", "fy"), P("ch", "fx", "fy"), P("ch", "fx", "fy"), P("fx", "fy")),
        out_specs=(P("ch", "fx", "fy"), P("ch", "fx", "fy")),
        check_vma=False,
    )
```

```python
import functools

import jax
import jax.numpy as jnp
import numpy as np
from jax import lax
from jax.experimental import pallas as pl
from jax.experimental.pallas import tpu as pltpu
from jax.sharding import PartitionSpec as P

LOW_PASS = [
    -0.00011747678400228192,
    0.0006754494059985568,
    -0.0003917403729959771,
    -0.00487035299301066,
    0.008746094047015655,
    0.013981027917015516,
    -0.04408825393106472,
    -0.01736930100202211,
    0.128747426620186,
    0.00047248457399797254,
    -0.2840155429624281,
    -0.015829105256023893,
    0.5853546836548691,
    0.6756307362980128,
    0.3128715909144659,
    0.05441584224308161,
]
TAU_STEP = 0.5
LAMBDA_REG = 1.0
EPSILON = 1e-06
LANES = 128
GROUP = 4
RUN = 4
RELAYED_LEFT = ((0, 1, 3, 4, 6), (1, 3, 5), (3,))
RELAYED_RIGHT = ((2, 6), (0, 2, 4, 6), (0, 1, 2, 4, 5, 6))
IMAGE_LAG = (5, 8)
ROWS_LAG = (13, 16)
RELAY_LAG = (3, 7)
MESH = pl.DeviceIdType.MESH


def level_matrix(length):
    halved = length // 2
    taps_count = len(LOW_PASS)
    matrix = np.zeros((length, length))
    for out_row in range(halved):
        for tap_index in range(taps_count):
            column = (2 * out_row + tap_index) % length
            matrix[out_row, column] += LOW_PASS[tap_index]
            matrix[halved + out_row, column] += (-1) ** tap_index * LOW_PASS[
                taps_count - 1 - tap_index
            ]
    return matrix


def split_np(matrix):
    single = matrix.astype(np.float32)
    high = single.astype(jnp.bfloat16)
    low = (single - high.astype(np.float32)).astype(jnp.bfloat16)
    return np.stack([high, low])


def matrices(ex, ey, border):
    wx, wy = level_matrix(ex), level_matrix(ey)
    hx, hy = ex // 2, ey // 2
    along_y = np.concatenate([level_matrix(hy) @ wy[:hy], wy], axis=0)
    order = np.concatenate([np.arange(border, ey), np.arange(border)])
    along_y = along_y[:, order]
    low_x = np.zeros((2 * ex, ex))
    low_x[:ex, :hx] = (level_matrix(hx) @ wx[:hx]).T
    low_x[ex:, hx:] = wx[hx:].T
    return [
        split_np(low_x),
        split_np(wx.T),
        split_np(along_y),
        split_np(along_y.T),
        split_np(low_x.T),
        split_np(wx),
    ]


def split(value):
    high = value.astype(jnp.bfloat16)
    low = (value - high.astype(jnp.float32)).astype(jnp.bfloat16)
    return high, low


def dot3(a, b):
    dot = functools.partial(jnp.dot, preferred_element_type=jnp.float32)
    return dot(a[0], b[0]) + (dot(a[0], b[1]) + dot(a[1], b[0]))


def kernel(
    sizes,
    img_hbm, grad_hbm, dual_hbm, rw_hbm, lowx_hbm, wxt_hbm, ay_hbm, ayt_hbm, lowxt_hbm, wx_hbm,
    image_next, updated, factor,
    img, grad, dual, rw, lowx, wxt, ay, ayt, lowxt, wx,
    work, rows_hi, rows_lo, mixed,
    fy1_s, fy1_r, bulk1_s, bulk1_r, corner1_s, corner1_r,
    bulk2_s, bulk2_r, corner2_s, corner2_r, fy2_s, fy2_r, via_bulk, via_corner, total, other,
    dual_sem, img_sem, grad_sem, const_sem,
    fy1_ss, fy1_rs, bulk1_ss, bulk1_rs, corner1_ss, corner1_rs,
    bulk2_ss, bulk2_rs, corner2_ss, corner2_rs, fy2_ss, fy2_rs,
    via_bulk_ss, via_bulk_rs, via_corner_ss, via_corner_rs, ch_ss, ch_rs,
):
    n_fx, n_fy, chunks, tx, ty, border = sizes
    ex = tx + border
    ey = ty + border
    tail = ty - LANES
    half = border // 2
    fx, fy, ch = lax.axis_index("fx"), lax.axis_index("fy"), lax.axis_index("ch")
    has_left, has_right = fx > 0, fx < n_fx - 1
    has_up, has_down = fy > 0, fy < n_fy - 1

    relays = n_fx == RUN * RUN
    run, place = fx // RUN, fx % RUN
    at_first, at_last = place == 0, place == RUN - 1
    if relays:
        crosses_left, crosses_right = at_first & has_left, at_last & has_right
        via1_here, via2_here = at_first & (run < RUN - 1), at_last & (run > 0)
    else:
        crosses_left = crosses_right = via1_here = via2_here = False

    def among(chosen, pair, k):
        found = False
        for index, listed in enumerate(chosen):
            for member in listed:
                found = found | ((pair == index) & (k == member))
        return found

    def by_relay(crosses, relayed, direct, relay, action):
        if not relays:
            return action(direct())
        pl.when(crosses & relayed)(lambda: action(relay()))
        pl.when(jnp.logical_not(crosses & relayed))(lambda: action(direct()))

    def left_relayed(k):
        return among(RELAYED_LEFT, run - 1, k)

    def right_relayed(k):
        return among(RELAYED_RIGHT, run, k)

    barrier = pltpu.get_barrier_semaphore()

    def greet(condition, where):
        @pl.when(condition)
        def _():
            pl.semaphore_signal(barrier, inc=1, device_id=where, device_id_type=MESH)

    greet(has_left, {"fx": fx - 1})
    greet(has_right, {"fx": fx + 1})
    greet(has_up, {"fy": fy - 1})
    greet(has_down, {"fy": fy + 1})
    pl.semaphore_signal(barrier, inc=1, device_id={"ch": 1 - ch}, device_id_type=MESH)
    neighbours = 1 + sum(c.astype(jnp.int32) for c in (has_left, has_right, has_up, has_down))
    if relays:
        ends = at_first | at_last
        for condition, offset in (
            (ends & (run > 0), -RUN), (ends & (run < RUN - 1), RUN), (at_first, RUN - 1), (at_last, 1 - RUN)
        ):
            greet(condition, {"fx": fx + offset})
            neighbours = neighbours + condition.astype(jnp.int32)

    def load(src, dst, sems, k):
        rows = pl.ds(k * GROUP, GROUP)
        return pltpu.make_async_copy(src.at[rows], dst.at[rows], sems.at[k])

    constants = [
        (lowx_hbm, lowx), (wxt_hbm, wxt), (ay_hbm, ay), (ayt_hbm, ayt), (lowxt_hbm, lowxt), (wx_hbm, wx), (rw_hbm, rw)
    ]

    def constant(i):
        return pltpu.make_async_copy(constants[i][0], constants[i][1], const_sem.at[i])

    load(dual_hbm, dual, dual_sem, 0).start()
    for i in range(3):
        constant(i).start()
    def clear(condition, *refs):
        @pl.when(condition)
        def _():
            for ref in refs:
                ref[...] = jnp.zeros_like(ref)

    clear(fy == n_fy - 1, fy1_r)
    clear(fx == n_fx - 1, bulk1_r, corner1_r)
    clear(fx == 0, bulk2_r, corner2_r)
    clear(fy == 0, fy2_r)
    total[...] = jnp.zeros_like(total)

    def remote(src, dst, send, recv, k, where):
        return pltpu.make_async_remote_copy(
            src_ref=src.at[k], dst_ref=dst.at[k], send_sem=send.at[k], recv_sem=recv.at[k],
            device_id=where, device_id_type=MESH,
        )

    def fy1(k):
        return remote(fy1_s, fy1_r, fy1_ss, fy1_rs, k, {"fy": fy - 1})

    def bulk1(k):
        return remote(bulk1_s, bulk1_r, bulk1_ss, bulk1_rs, k, {"fx": fx - 1})

    def corner1(k):
        return remote(corner1_s, corner1_r, corner1_ss, corner1_rs, k, {"fx": fx - 1})

    def bulk2(k):
        return remote(bulk2_s, bulk2_r, bulk2_ss, bulk2_rs, k, {"fx": fx + 1})

    def corner2(k):
        return remote(corner2_s, corner2_r, corner2_ss, corner2_rs, k, {"fx": fx + 1})

    def to_relay(src, via, send, recv, k, offset):
        return remote(src, via, send, recv, k, {"fx": fx + offset})

    def via_bulk1(k):
        return to_relay(bulk1_s, via_bulk, bulk1_ss, via_bulk_rs, k, -RUN)

    def via_corner1(k):
        return to_relay(corner1_s, via_corner, corner1_ss, via_corner_rs, k, -RUN)

    def via_bulk2(k):
        return to_relay(bulk2_s, via_bulk, bulk2_ss, via_bulk_rs, k, RUN)

    def via_corner2(k):
        return to_relay(corner2_s, via_corner, corner2_ss, via_corner_rs, k, RUN)

    def on_bulk1(k):
        return to_relay(via_bulk, bulk1_r, via_bulk_ss, bulk1_rs, k, RUN - 1)

    def on_corner1(k):
        return to_relay(via_corner, corner1_r, via_corner_ss, corner1_rs, k, RUN - 1)

    def on_bulk2(k):
        return to_relay(via_bulk, bulk2_r, via_bulk_ss, bulk2_rs, k, 1 - RUN)

    def on_corner2(k):
        return to_relay(via_corner, corner2_r, via_corner_ss, corner2_rs, k, 1 - RUN)

    def leftward(direct, relay, k, action):
        pl.when(has_left)(lambda: by_relay(crosses_left, left_relayed(k), lambda: direct(k), lambda: relay(k), action))

    def rightward(direct, relay, k, action):
        pl.when(has_right)(lambda: by_relay(crosses_right, right_relayed(k), lambda: direct(k), lambda: relay(k), action))

    def start(copy):
        copy.start()

    def wait_send(copy):
        copy.wait_send()

    def carries1(k):
        return via1_here & among(RELAYED_LEFT, run, k)

    def carries2(k):
        return via2_here & among(RELAYED_RIGHT, run - 1, k)

    def relay1(k):
        @pl.when(carries1(k))
        def _():
            via_bulk1(k).wait_recv()
            on_bulk1(k).start()
            via_corner1(k).wait_recv()
            on_corner1(k).start()

    def relay2(k):
        @pl.when(carries2(k))
        def _():
            via_corner2(k).wait_recv()
            on_corner2(k).start()
            via_bulk2(k).wait_recv()
            on_bulk2(k).start()

    def fy2(k):
        return remote(fy2_s, fy2_r, fy2_ss, fy2_rs, k, {"fy": fy + 1})

    lane_e = lax.broadcasted_iota(jnp.int32, (ex, LANES), 1)
    lane_b = lax.broadcasted_iota(jnp.int32, (border, LANES), 1)
    lane_h = lax.broadcasted_iota(jnp.int32, (half, LANES), 1)
    low_edge = (lane_e >= tail - border) & (lane_e < tail)

    def roll(value, shift):
        shift = shift % LANES
        return pltpu.roll(value, shift, 1) if shift else value

    def pack_bulk(tile0, tile1, out, k):
        joined = jnp.zeros((border, LANES), jnp.float32)
        for c in range(GROUP):
            out[k, c * border : (c + 1) * border, :] = tile0(c)
            moved = roll(tile1(c), 32 * c)
            joined = jnp.where((lane_b >= 32 * c) & (lane_b < 32 * c + 32), moved, joined)
        out[k, GROUP * border : (GROUP + 1) * border, :] = joined

    def pack_corner(tile1, out, k):
        joined = jnp.zeros((border, LANES), jnp.float32)
        rest = jnp.zeros((half, LANES), jnp.float32)
        for c in range(GROUP):
            value = tile1(c)
            moved = roll(value, 32 * c - 32)
            joined = jnp.where((lane_b >= 32 * c) & (lane_b < 32 * c + 32), moved, joined)
            for part in range(2):
                to = part * 64 + c * 16
                moved = roll(value[part * half : (part + 1) * half], to - 64)
                rest = jnp.where((lane_h >= to) & (lane_h < to + 16), moved, rest)
        out[k, :border, :] = joined
        out[k, border:, :] = rest

    def unpack_corner(ref, k, c):
        middle = roll(ref[k, :border, :], 32 - 32 * c)
        parts = [roll(ref[k, border:, :], 64 - part * 64 - c * 16) for part in range(2)]
        return jnp.where(lane_b < 64, middle, jnp.concatenate(parts, axis=0))

    def unpack(bulk, corner, k, c):
        first = bulk[k, c * border : (c + 1) * border, :]
        start = roll(bulk[k, GROUP * border : (GROUP + 1) * border, :], -32 * c)
        return first, jnp.where(lane_b < 32, start, unpack_corner(corner, k, c))

    def put_rows(at, lanes, value):
        high = value.astype(jnp.bfloat16)
        rows = slice(at, at + value.shape[0])
        rows_hi[rows, lanes] = high
        rows_lo[rows, lanes] = (value - high.astype(jnp.float32)).astype(jnp.bfloat16)

    def put_edge_first(c, tile, value):
        lanes = slice(tile * LANES, (tile + 1) * LANES)
        put_rows(c * border, lanes, value[:border])
        put_rows(GROUP * border + c * tx, lanes, value[border:])

    def synthesize(k):
        load(dual_hbm, dual, dual_sem, k).wait()
        first = k * GROUP
        left = jnp.concatenate([dual[first + c, :, :LANES] for c in range(GROUP)], axis=1)
        from_left = dot3((lowx[0], lowx[1]), split(left))
        for c in range(GROUP):
            lanes = slice(c * LANES, (c + 1) * LANES)
            put_edge_first(c, 0, from_left[:ex, lanes])
            put_edge_first(c, 1, from_left[ex:, lanes])
        right = jnp.concatenate([dual[first + c, :, LANES:] for c in range(GROUP)], axis=1)
        from_right = dot3((wxt[0], wxt[1]), split(right))
        for c in range(GROUP):
            put_edge_first(c, 2, from_right[:, c * LANES : (c + 1) * LANES])
        edges = GROUP * border
        result = dot3((rows_hi[:edges], rows_lo[:edges]), (ay[0], ay[1]))
        for c in range(GROUP):
            work[first + c, :border] = result[c * border : (c + 1) * border]

        @pl.when(k == 0)
        def _():
            pl.semaphore_wait(barrier, neighbours)
            send_bulk(k)

        result = dot3((rows_hi[edges:], rows_lo[edges:]), (ay[0], ay[1]))
        for c in range(GROUP):
            work[first + c, border:] = result[c * tx : (c + 1) * tx]
        for p in range(GROUP // 2):
            a, b = work[first + 2 * p, :, LANES:], work[first + 2 * p + 1, :, LANES:]
            fy1_s[k, p] = jnp.where(low_edge, roll(a, -border), roll(b, 64 - border))
        pl.when(has_up)(lambda: fy1(k).start())

    def send_bulk(k):
        first = k * GROUP
        pack_bulk(
            lambda c: work[first + c, :border, :LANES], lambda c: work[first + c, :border, LANES:], bulk1_s, k
        )
        leftward(bulk1, via_bulk1, k, start)

    def send_later_bulk(k):
        pl.when(k > 0)(lambda: send_bulk(k))

    def send_columns(k):
        pl.when(has_down)(lambda: fy1(k).wait_recv())
        for p in range(GROUP // 2):
            a = k * GROUP + 2 * p
            strip = fy1_r[k, p]
            work[a, :, LANES:] = work[a, :, LANES:] + jnp.where(low_edge, strip, 0.0)
            work[a + 1, :, LANES:] = work[a + 1, :, LANES:] + jnp.where(low_edge, roll(strip, 64), 0.0)
        pack_corner(lambda c: work[k * GROUP + c, :border, LANES:], corner1_s, k)
        leftward(corner1, via_corner1, k, start)

    root = jnp.float32(0.5**0.5)

    def weights(lane_from):
        rows = lax.broadcasted_iota(jnp.int32, (tx, LANES), 0)
        lanes = lax.broadcasted_iota(jnp.int32, (tx, LANES), 1) + lane_from
        by_x = jnp.where((rows >= tx - border) & has_right, root, 1.0)
        by_y = jnp.where((lanes >= ty - border) & has_down, root, 1.0)
        return by_x * by_y

    def update_image(k):
        load(img_hbm, img, img_sem, k).wait()
        load(grad_hbm, grad, grad_sem, k).wait()

        @pl.when(has_right)
        def _():
            bulk1(k).wait_recv()
            corner1(k).wait_recv()

        keep = tx - border
        w0 = weights(0)
        w1 = weights(LANES)[:, :tail]
        for c in range(GROUP):
            i = k * GROUP + c
            add0, add1 = unpack(bulk1_r, corner1_r, k, c)
            for own, add, w, lanes in (
                (work[i, border:, :LANES], add0, w0, slice(0, LANES)),
                (work[i, border:, LANES:ty], add1[:, :tail], w1, slice(LANES, ty)),
            ):
                summed = jnp.concatenate([own[:keep], own[keep:] + add], axis=0)
                image = img[i, :, lanes]
                step = jnp.maximum(image - TAU_STEP * (grad[i, :, lanes].astype(jnp.float32) + summed * w), 0.0)
                image_next[i, :, lanes] = step
                work[i, border:, lanes] = (2.0 * step - image) * w
        pack_corner(lambda c: work[k * GROUP + c, tx:, LANES:], corner2_s, k)
        rightward(corner2, via_corner2, k, start)
        pack_bulk(
            lambda c: work[k * GROUP + c, tx:, :LANES], lambda c: work[k * GROUP + c, tx:, LANES:], bulk2_s, k
        )
        rightward(bulk2, via_bulk2, k, start)

    def send_rows(k):
        pl.when(has_left)(lambda: corner2(k).wait_recv())
        for p in range(GROUP // 2):
            a, b = [
                jnp.concatenate([unpack_corner(corner2_r, k, c), work[k * GROUP + c, border:, LANES:]], axis=0)
                for c in (2 * p, 2 * p + 1)
            ]
            fy2_s[k, p] = jnp.where(lane_e >= tail, roll(a, border), roll(b, 64 + border))
        pl.when(has_down)(lambda: fy2(k).start())

    def analyse(k):
        @pl.when(k == 0)
        def _():
            for i in range(3, len(constants)):
                constant(i).wait()

        pl.when(has_left)(lambda: bulk2(k).wait_recv())
        pl.when(has_up)(lambda: fy2(k).wait_recv())
        first = k * GROUP
        for c in range(GROUP):
            i = first + c
            strip = roll(fy2_r[k, c // 2], 64 * (c % 2))
            edge0, edge1 = unpack(bulk2_r, corner2_r, k, c)
            put_rows(c * ex, slice(0, LANES), jnp.concatenate([edge0, work[i, border:, :LANES]], axis=0))
            second = jnp.concatenate([edge1, work[i, border:, LANES:]], axis=0)
            put_rows(c * ex, slice(LANES, 2 * LANES), jnp.where(lane_e < tail, second, strip))
        mixed[...] = dot3((rows_hi[:, :ey], rows_lo[:, :ey]), (ayt[0], ayt[1]))

        def beside(tile):
            lanes = slice(tile * LANES, (tile + 1) * LANES)
            return jnp.concatenate([mixed[c * ex : (c + 1) * ex, lanes] for c in range(GROUP)], axis=1)

        low = dot3((lowxt[0], lowxt[1]), split(jnp.concatenate([beside(0), beside(1)], axis=0)))
        high = dot3((wx[0], wx[1]), split(beside(2)))
        for lanes, part in ((slice(0, LANES), low), (slice(LANES, 2 * LANES), high)):
            squares = total[:, lanes]
            for c in range(GROUP):
                value = dual[first + c, :, lanes] + part[:, c * LANES : (c + 1) * LANES]
                updated[first + c, :, lanes] = value
                squares = squares + value * value
            total[:, lanes] = squares

    for i in range(3):
        constant(i).wait()
    for k in range(1, chunks):
        load(dual_hbm, dual, dual_sem, k).start()
    for k in range(chunks):
        load(img_hbm, img, img_sem, k).start()
        load(grad_hbm, grad, grad_sem, k).start()
    for i in range(3, len(constants)):
        constant(i).start()

    image_lag, rows_lag = [jnp.where(crosses_right, *lags) for lags in (IMAGE_LAG, ROWS_LAG)]
    phases = (
        (synthesize, 0), (send_columns, 2), (send_later_bulk, 0), (relay1, RELAY_LAG[0]), (update_image, image_lag),
        (relay2, RELAY_LAG[1]), (send_rows, rows_lag), (analyse, rows_lag + 1),
    )
    if not relays:
        phases = tuple(p for p in phases if p[0] not in (relay1, relay2))

    def step(s, carry):
        for phase, lag in phases:

            @pl.when((s >= lag) & (s < chunks + lag))
            def _(phase=phase, lag=lag):
                phase(s - lag)

        return carry

    lax.fori_loop(0, chunks + rows_lag + 1, step, 0)

    swap = pltpu.make_async_remote_copy(
        src_ref=total, dst_ref=other, send_sem=ch_ss, recv_sem=ch_rs, device_id={"ch": 1 - ch}, device_id_type=MESH
    )
    swap.start()

    def drain(k, carry):
        pl.when(has_up)(lambda: fy1(k).wait_send())

        leftward(bulk1, via_bulk1, k, wait_send)
        leftward(corner1, via_corner1, k, wait_send)
        rightward(corner2, via_corner2, k, wait_send)
        rightward(bulk2, via_bulk2, k, wait_send)
        if relays:

            @pl.when(carries1(k))
            def _():
                on_bulk1(k).wait_send()
                on_corner1(k).wait_send()

            @pl.when(carries2(k))
            def _():
                on_bulk2(k).wait_send()
                on_corner2(k).wait_send()

        pl.when(has_down)(lambda: fy2(k).wait_send())
        return carry

    lax.fori_loop(0, chunks, drain, 0)
    swap.wait()
    factor[...] = jnp.minimum(1.0, LAMBDA_REG * rw[...] / jnp.sqrt(total[...] + other[...] + EPSILON))


def finish(chunks, image, updated, factor, image_out, dual_out, scaled, image_sem, sems):
    pltpu.make_async_copy(image, image_out, image_sem).start()

    def copy(k):
        rows = pl.ds(k * GROUP, GROUP)
        return pltpu.make_async_copy(scaled.at[rows], dual_out.at[rows], sems.at[k])

    def step(k, carry):
        for c in range(GROUP):
            scaled[k * GROUP + c] = updated[k * GROUP + c] * factor[...]
        copy(k).start()
        return carry

    lax.fori_loop(0, chunks, step, 0)
    pltpu.make_async_copy(image, image_out, image_sem).wait()

    def drain(k, carry):
        copy(k).wait()
        return carry

    lax.fori_loop(0, chunks, drain, 0)


def shards(mesh_shape, image_cube, data_grad, dual_coeffs, reweights):
    channels, tx, ty = image_cube.shape
    _, ex, ey = dual_coeffs.shape
    border = ex - tx
    chunks = channels // GROUP
    constants = [jnp.asarray(m) for m in matrices(ex, ey, border)]
    sizes = (mesh_shape["fx"], mesh_shape["fy"], chunks, tx, ty, border)
    f32, bf16 = jnp.float32, jnp.bfloat16
    strip_y = pltpu.VMEM((chunks, GROUP // 2, ex, LANES), f32)
    bulk = pltpu.VMEM((chunks, (GROUP + 1) * border, LANES), f32)
    corner = pltpu.VMEM((chunks, border + border // 2, LANES), f32)
    dma = pltpu.SemaphoreType.DMA
    in_hbm = pl.BlockSpec(memory_space=pltpu.HBM)
    in_vmem = pl.BlockSpec(memory_space=pltpu.VMEM)
    operands = [
        pltpu.with_memory_space_constraint(x, pltpu.HBM)
        for x in (image_cube, data_grad, dual_coeffs, reweights, *constants)
    ]
    image_next, updated, factor = pl.pallas_call(
        functools.partial(kernel, sizes),
        out_shape=(
            jax.ShapeDtypeStruct(image_cube.shape, f32),
            jax.ShapeDtypeStruct(dual_coeffs.shape, f32),
            jax.ShapeDtypeStruct(reweights.shape, f32),
        ),
        in_specs=[in_hbm] * len(operands),
        out_specs=(in_vmem,) * 3,
        scratch_shapes=[
            pltpu.VMEM(image_cube.shape, f32),
            pltpu.VMEM(data_grad.shape, data_grad.dtype),
            pltpu.VMEM(dual_coeffs.shape, f32),
            pltpu.VMEM(reweights.shape, f32),
            *[pltpu.VMEM(m.shape, m.dtype) for m in constants],
            pltpu.VMEM(dual_coeffs.shape, f32),
            pltpu.VMEM((GROUP * ex, ey + LANES), bf16),
            pltpu.VMEM((GROUP * ex, ey + LANES), bf16),
            pltpu.VMEM((GROUP * ex, ey + LANES), f32),
            strip_y, strip_y, bulk, bulk, corner, corner, bulk, bulk, corner, corner, strip_y, strip_y, bulk, corner,
            pltpu.VMEM((ex, ey), f32), pltpu.VMEM((ex, ey), f32),
            dma((chunks,)), dma((chunks,)), dma((chunks,)), dma((7,)),
            *[dma((chunks,)) for _ in range(16)],
            dma, dma,
        ],
        compiler_params=pltpu.CompilerParams(
            collective_id=0, has_side_effects=True, vmem_limit_bytes=40 * 2**20
        ),
        name="primal_dual",
    )(*operands)
    return pl.pallas_call(
        functools.partial(finish, chunks),
        out_shape=(
            jax.ShapeDtypeStruct(image_cube.shape, f32),
            jax.ShapeDtypeStruct(dual_coeffs.shape, f32),
        ),
        in_specs=[in_vmem] * 3,
        out_specs=(in_hbm,) * 2,
        scratch_shapes=[pltpu.VMEM(dual_coeffs.shape, f32), dma, dma((chunks,))],
        compiler_params=pltpu.CompilerParams(vmem_limit_bytes=16 * 2**20),
        name="scaled_results",
    )(image_next, updated, factor)


def solution(mesh):
    return jax.shard_map(
        functools.partial(shards, dict(mesh.shape)),
        mesh=mesh,
        in_specs=(P("ch", "fx", "fy"), P("ch", "fx", "fy"), P("ch", "fx", "fy"), P("fx", "fy")),
        out_specs=(P("ch", "fx", "fy"), P("ch", "fx", "fy")),
        check_vma=False,
    )
```
